512 devices in a mesh: dp: 4 (over y), tensor: 8 (over z_hi, x), enc: 16 (over z_lo, core).
Axes of the slice: x: 4, y: 4, z: 16 (z_hi: 2, z_lo: 8; z = z_hi * 8 + z_lo), core: 2. Of those that a mesh axis runs over, the one named last changes fastest.
Arguments:
- span_states: bfloat16 [8192, 8192], P(('dp', 'enc'), 'tensor'), may hold values from -6 to 6
- neighbours: bfloat16 [128, 256, 1024], P(('dp', 'enc'), None, 'tensor'), may hold values from -6 to 6
- lengths: int32 [4], P('dp'), may hold values from 1 to 2048, 4096 in all
- wq_enc: bfloat16 [1024, 1024], P('enc', 'tensor')
- wk_enc: bfloat16 [8192, 1024], P('enc', 'tensor'), may hold values from -0.0625 to 0.0625
- wv_enc: bfloat16 [8192, 1024], P('enc', 'tensor'), may hold values from -0.0625 to 0.0625
- wo_enc: bfloat16 [1024, 1024], P('enc', 'tensor'), may hold values from -0.1875 to 0.1875
- wk_dec: bfloat16 [1024, 8192], P(('dp', 'enc'), 'tensor'), may hold values from -0.1875 to 0.1875
- wv_dec: bfloat16 [1024, 8192], P(('dp', 'enc'), 'tensor'), may hold values from -0.1875 to 0.1875
- queries: bfloat16 [8192, 8192], P(('dp', 'enc'), 'tensor'), may hold values from -6 to 6
- grad_out: bfloat16 [8192, 8192], P(('dp', 'enc'), 'tensor'), may hold values from -6 to 6
Outputs:
- attended: bfloat16 [8192, 8192], P(('dp', 'enc'), 'tensor')
- grad_encoded: float32 [128, 256, 1024], P(('dp', 'enc'), None, 'tensor')
The draws below stay inside these ranges and needn't reach their ends.
Inputs may be any that keep to these rules, and one draw needn't show every extreme that they name: `lengths`: some sequence is live over all 2048 tokens.
All inputs are finite; a program needn't handle non-finite values. No bound on the sum of `lengths` on one device may be relied on, other than what follows from the above.
Results may differ from the reference program's by a relative error of at most 0.019.
Values may be sent and summed in bfloat16 or wider, within the bound.
A program may use at most 64 MiB of HBM per device.

```python
import math
import jax
import jax.numpy as jnp
import numpy as np
from jax import lax

D = 8192
HD = 128
DE = 1024
EH = 64
M = 64
NB = 2
R = 128
SEQ_LEN = 2048
SEQS = 4
SPANS = 128
TOKENS = 8192


def draw_wq_enc(key, part):
    own_key = jax.random.fold_in(key, 101)
    values = jnp.clip(jax.random.normal(own_key, (DE, DE), jnp.float32), -6.0, 6.0) / math.sqrt(DE)
    return values.astype(jnp.bfloat16)


def draw_queries(key, part):
    own_key = jax.random.fold_in(key, 202)
    values = jnp.clip(jax.random.normal(own_key, (TOKENS, D), jnp.float32), -6.0, 6.0)
    return values.astype(jnp.bfloat16)


def steps_of(stream_key, extent, cuts, least, high):
    loudness = 1.0
    for axis_at, parts in cuts:
        steps = jax.random.uniform(jax.random.fold_in(jax.random.fold_in(stream_key, 6), axis_at), (parts,), jnp.float32, least / len(cuts), high / len(cuts))
        loudness = loudness * jnp.repeat(jnp.exp(steps), extent[axis_at] // parts).reshape((-1,) + (1,) * (len(extent) - 1 - axis_at))
    return loudness


def length_profile(amount, total, bound, lean):
    loads = [(1 << 20) // math.isqrt(standing ** lean) + 1 for standing in range(2, amount + 1)]
    rest, holding = total - bound - (amount - 1), [1] * (amount - 1)
    while rest > 0:
        free = [i for i in range(amount - 1) if holding[i] < bound]
        whole, budget = sum([loads[i] for i in free]), rest
        for i in free:
            more = min(bound - holding[i], max(1, budget * loads[i] // whole), rest)
            holding[i] = holding[i] + more
            rest = rest - more
    return np.array([bound] + holding)


def uneven_parts(stream_key, number_of, total, most, slope):
    if number_of == 2:
        one = jax.random.randint(stream_key, (), max(1, total - most), min(most, total - 1) + 1)
        return jnp.stack([one, total - one])
    tallies = jnp.asarray(length_profile(number_of, total, most, slope), jnp.int32)
    couples = (number_of - 1) // 2
    source_of, sink = tallies[1:1 + 2 * couples:2], tallies[2:2 + 2 * couples:2]
    room = jnp.minimum(source_of - 1, most - sink)
    shifted = jax.random.randint(jax.random.fold_in(stream_key, 1), (couples,), 0, 1 << 20) % (room + 1)
    tallies = tallies.at[1:1 + 2 * couples:2].set(source_of - shifted).at[2:2 + 2 * couples:2].set(sink + shifted)
    return tallies[jax.random.permutation(jax.random.fold_in(stream_key, 2), number_of)]


def normal_values(stream_key, extent, spread, bound, cuts=(), kind=jnp.bfloat16):
    array = jax.random.normal(stream_key, extent, jnp.float32) * spread
    if len(cuts) > 0:
        array = steps_of(stream_key, extent, cuts, -0.22, 0.18) * array
    return jnp.clip(array, min=-bound, max=bound).astype(kind)


def setup_inputs(seed: int = 0) -> dict:
    splits = jax.random.split(jax.random.key(seed), 12)
    return {
        "span_states": normal_values(splits[0], (TOKENS, D), 1.0, 6.0, ((0, 64), (1, 8))),
        "neighbours": normal_values(splits[1], (SPANS, NB * R, DE), 1.0, 6.0, ((0, 64), (2, 8))),
        "lengths": uneven_parts(splits[2], SEQS, SEQS * SEQ_LEN // 2, SEQ_LEN, 2).astype(jnp.int32),
        "wq_enc": draw_wq_enc(jax.random.fold_in(splits[11], 71), 0),
        "wk_enc": normal_values(splits[4], (D, DE), D ** -0.5, 0.0625, ((0, 16), (1, 8))),
        "wv_enc": normal_values(splits[5], (D, DE), D ** -0.5, 0.0625, ((0, 16), (1, 8))),
        "wo_enc": normal_values(splits[6], (DE, DE), DE ** -0.5, 0.1875, ((0, 16), (1, 8))),
        "wk_dec": normal_values(splits[7], (DE, D), DE ** -0.5, 0.1875, ((0, 64), (1, 8))),
        "wv_dec": normal_values(splits[8], (DE, D), DE ** -0.5, 0.1875, ((0, 64), (1, 8))),
        "queries": draw_queries(jax.random.fold_in(splits[11], 71), 0),
        "grad_out": normal_values(splits[10], (TOKENS, D), 1.0, 6.0, ((0, 64), (1, 8))),
    }


def one_sequence(states, neighbour, length, queries, grad_out, wq_enc, wk_enc, wv_enc, wo_enc, wk_dec, wv_dec):
    count = SEQ_LEN // M
    keys_each = NB * R
    flat_neighbour = neighbour.reshape(count * keys_each, DE)
    enc_query = jnp.dot(flat_neighbour, wq_enc, preferred_element_type=jnp.float32).astype(jnp.bfloat16)
    enc_key = jnp.dot(states, wk_enc, preferred_element_type=jnp.float32).astype(jnp.bfloat16)
    enc_value = jnp.dot(states, wv_enc, preferred_element_type=jnp.float32).astype(jnp.bfloat16)
    query_heads = enc_query.reshape(count, keys_each, DE // EH, EH).astype(jnp.float32)
    key_heads = enc_key.reshape(count, M, DE // EH, EH).astype(jnp.float32)
    value_heads = enc_value.reshape(count, M, DE // EH, EH).astype(jnp.float32)
    scores = jnp.einsum('cqhe,ckhe->chqk', query_heads, key_heads) / math.sqrt(EH)
    enc_weights = jax.nn.softmax(scores, axis=-1).astype(jnp.bfloat16)
    head_mix = jnp.einsum('chqk,ckhe->cqhe', enc_weights.astype(jnp.float32), value_heads)
    head_mix = head_mix.astype(jnp.bfloat16).reshape(count * keys_each, DE)
    encoded = flat_neighbour.astype(jnp.float32) + jnp.dot(head_mix, wo_enc, preferred_element_type=jnp.float32)
    encoded = encoded.astype(jnp.bfloat16).reshape(count, keys_each, DE)
    previous = jnp.concatenate([jnp.zeros((1, keys_each, DE), jnp.bfloat16), encoded[:-1]], axis=0)
    previous = previous.reshape(count * keys_each, DE)
    dec_key = jnp.dot(previous, wk_dec, preferred_element_type=jnp.float32).astype(jnp.bfloat16)
    dec_value = jnp.dot(previous, wv_dec, preferred_element_type=jnp.float32).astype(jnp.bfloat16)
    heads_dec = D // HD
    query_dec = queries.reshape(count, M, heads_dec, HD).astype(jnp.float32)
    key_dec = dec_key.reshape(count, keys_each, heads_dec, HD).astype(jnp.float32)
    value_dec = dec_value.reshape(count, keys_each, heads_dec, HD).astype(jnp.float32)
    dec_scores = jnp.einsum('cmhd,ckhd->chmk', query_dec, key_dec) / math.sqrt(HD)
    probs = jax.nn.softmax(dec_scores, axis=-1)
    probs_low = probs.astype(jnp.bfloat16)
    position = jnp.arange(SEQ_LEN, dtype=jnp.int32)
    live_mask = jnp.logical_and(position < length, position >= M).reshape(count, M, 1, 1)
    attended = jnp.einsum('chmk,ckhd->cmhd', probs_low.astype(jnp.float32), value_dec)
    attended = jnp.where(live_mask, attended, 0.0).astype(jnp.bfloat16).reshape(SEQ_LEN, D)
    cotangent = jnp.where(live_mask, grad_out.reshape(count, M, heads_dec, HD), jnp.zeros((), jnp.bfloat16))
    cot_float = cotangent.astype(jnp.float32)
    grad_value = jnp.einsum('chmk,cmhd->ckhd', probs_low.astype(jnp.float32), cot_float).astype(jnp.bfloat16)
    grad_probs = jnp.einsum('cmhd,ckhd->chmk', cot_float, value_dec)
    inner = lax.optimization_barrier(jnp.sum(grad_probs * probs, axis=-1, keepdims=True))
    grad_scores = (probs * (grad_probs - inner) / math.sqrt(HD)).astype(jnp.bfloat16)
    grad_key = jnp.einsum('chmk,cmhd->ckhd', grad_scores.astype(jnp.float32), query_dec).astype(jnp.bfloat16)
    grad_previous = jnp.dot(grad_key.reshape(count * keys_each, D), wk_dec.T, preferred_element_type=jnp.float32)
    grad_previous = grad_previous + jnp.dot(grad_value.reshape(count * keys_each, D), wv_dec.T, preferred_element_type=jnp.float32)
    grad_previous = grad_previous.reshape(count, keys_each, DE)
    grad_encoded = jnp.concatenate([grad_previous[1:], jnp.zeros((1, keys_each, DE), jnp.float32)], axis=0)
    return (attended, grad_encoded)

def reference(span_states, neighbours, lengths, wq_enc, wk_enc, wv_enc, wo_enc, wk_dec, wv_dec, queries, grad_out):
    count = SEQ_LEN // M
    seq_states = span_states.reshape(SEQS, SEQ_LEN, D)
    seq_neighbours = neighbours.reshape(SEQS, count, NB * R, DE)
    seq_queries = queries.reshape(SEQS, SEQ_LEN, D)
    seq_grads = grad_out.reshape(SEQS, SEQ_LEN, D)

    def per_sequence(items):
        return one_sequence(items[0], items[1], items[2], items[3], items[4], wq_enc, wk_enc, wv_enc, wo_enc, wk_dec, wv_dec)
    attended, grad_encoded = lax.map(per_sequence, (seq_states, seq_neighbours, lengths, seq_queries, seq_grads))
    return (attended.reshape(TOKENS, D), grad_encoded.reshape(SPANS, NB * R, DE))
```

```python
import math

import jax
import jax.numpy as jnp
from jax import lax
from jax.experimental import pallas as pl
from jax.experimental.pallas import tpu as pltpu
from jax.sharding import PartitionSpec as P

MESH = pl.DeviceIdType.MESH
BF = jnp.bfloat16
F32 = jnp.float32
NT = (((1,), (1,)), ((), ()))
TN = (((0,), (0,)), ((), ()))
NN = (((1,), (0,)), ((), ()))


def dot(a, b, dims=NN):
    return lax.dot_general(a, b, dims, preferred_element_type=F32)


def remote(src, dst, send, recv, device):
    return pltpu.make_async_remote_copy(
        src_ref=src, dst_ref=dst, send_sem=send, recv_sem=recv, device_id=device, device_id_type=MESH
    )


class Ring4:
    def __init__(self, me, device, full, half, send, recv, source=None):
        left, right, far = lax.rem(me + 3, 4), lax.rem(me + 1, 4), lax.rem(me + 2, 4)
        source = full(me) if source is None else source
        self.first = [
            remote(source, full(me), send.at[0], recv.at[0], device(right)),
            remote(source, full(me), send.at[1], recv.at[1], device(left)),
        ]
        self.arrive = [
            remote(full(left), full(left), send.at[0], recv.at[0], device(right)),
            remote(full(right), full(right), send.at[1], recv.at[1], device(left)),
        ]
        self.second = [
            remote(half(left, 0), half(left, 0), send.at[2], recv.at[2], device(right)),
            remote(half(right, 1), half(right, 1), send.at[3], recv.at[3], device(left)),
        ]
        self.last = [
            remote(half(far, 0), half(far, 0), send.at[2], recv.at[2], device(right)),
            remote(half(far, 1), half(far, 1), send.at[3], recv.at[3], device(left)),
        ]

    def start(self):
        for copy in self.first:
            copy.start()

    def middle(self):
        for k in range(2):
            self.arrive[k].wait_recv()
            self.second[k].start()

    def finish(self):
        for copy in self.last:
            copy.wait_recv()

    def drain(self):
        for copy in self.first + self.second:
            copy.wait_send()


def kernel(
    lens, s, n, q, g, wk, wv, wq, wo, wkd, wvd,
    att_out, grad_out,
    we, wqo, wd, sx, nx, qd, gd, mix, prev, gkv, att, part, precv, gsend, grecv,
    lsem, zs, zr, ys, yr, ds, dr, xs, xr, hs, hr, qs, qr, rs, rr, as_, ar,
):
    y, t, e = lax.axis_index("dp"), lax.axis_index("tensor"), lax.axis_index("enc")
    h, x = lax.div(t, 4), lax.rem(t, 4)
    j, c = lax.div(e, 2), lax.rem(e, 2)
    z = h * 8 + j
    before, after = lax.rem(e + 15, 16), lax.rem(e + 1, 16)
    sibling = (y, t, j * 2 + 1 - c)
    partner = (y, (1 - h) * 4 + x, e)

    def along_x(i):
        return (y, h * 4 + i, e)

    def along_y(i):
        return (i, t, e)

    def z_of(k):
        zz = lax.rem(z + k + 16, 16)
        return lax.div(zz, 8), lax.rem(zz, 8)

    def along_z(k):
        hz, jz = z_of(k)
        return (y, hz * 4 + x, jz * 2 + c)

    def lanes(i, width):
        return pl.ds(pl.multiple_of(i * width, width), width)

    blocks = (
        lambda b, yy: we.at[b[0], b[1], c, yy],
        lambda b, yy: wqo.at[b[0], b[1], c, yy],
        lambda b, yy: wd.at[b[0], yy, b[1], c],
    )
    whole = (
        lambda yy, cc: we.at[:, :, cc, yy],
        lambda yy, cc: wqo.at[:, :, cc, yy],
        lambda yy, cc: wd.at[:, yy, :, cc],
    )
    halves = (
        lambda yy, k: we.at[k, :, c, yy],
        lambda yy, k: wqo.at[k, :, c, yy],
        lambda yy, k: wd.at[k, yy, :, c],
    )
    kinds = range(3)
    own = (h, j)

    fetch = []

    def local(src, dst):
        copy = pltpu.make_async_copy(src, dst, lsem.at[len(fetch)])
        copy.start()
        fetch.append(copy)

    local(wk.at[pl.ds(y * 128, 128)], we.at[h, j, c, y, :, 0:128])
    local(wv.at[pl.ds(y * 128, 128)], we.at[h, j, c, y, :, 128:256])
    local(wq.at[pl.ds(y * 16, 16)], wqo.at[h, j, c, y, :, 0:128])
    local(wo.at[pl.ds(y * 16, 16)], wqo.at[h, j, c, y, :, 128:256])
    local(wkd, wd.at[h, y, j, c, :, 0:1024])
    local(wvd, wd.at[h, y, j, c, :, 1024:2048])
    local(s.at[pl.ds(h * 64, 64)], sx.at[t])
    local(n.at[h], nx.at[:, lanes(t, 128)])

    home = [
        pltpu.make_async_copy(q.at[64:128], qd.at[0], lsem.at[8]),
        pltpu.make_async_copy(g.at[64:128], gd.at[0], lsem.at[9]),
    ]

    @pl.when(h == 0)
    def _():
        for copy in home:
            copy.start()

    barrier = pltpu.get_barrier_semaphore()

    def greet(device):
        pl.semaphore_signal(barrier, inc=1, device_id=device, device_id_type=MESH)

    for k in (1, 2, 3):
        greet(along_x(lax.rem(x + k, 4)))
    for k in (1, 3):
        greet(along_y(lax.rem(y + k, 4)))
    for k in (1, -1):
        greet(along_z(k))
    greet(sibling)
    greet(partner)
    greet((y, 4 + x, before))

    @pl.when(h == 1)
    def _():
        greet((y, x, after))
        greet((y, 4 + x, after))

    pl.semaphore_wait(barrier, 10 + 2 * h)

    swaps = [
        remote(s.at[pl.ds((1 - h) * 64, 64)], sx.at[t], hs.at[0], hr.at[0], partner),
        remote(n.at[1 - h], nx.at[:, lanes(t, 128)], hs.at[1], hr.at[1], partner),
    ]
    for copy in swaps:
        copy.start()

    def s_ring(half_of, k, source=None):
        return Ring4(
            x, along_x,
            lambda i: sx.at[half_of * 4 + i],
            lambda i, m: sx.at[half_of * 4 + i, m * 32 : m * 32 + 32],
            xs.at[k], xr.at[k], source,
        )

    def wide_ring(ref, half_of, k, source=None):
        return Ring4(
            x, along_x,
            lambda i: ref.at[:, lanes(half_of * 4 + i, 128)],
            lambda i, m: ref.at[m * 128 : m * 128 + 128, lanes(half_of * 4 + i, 128)],
            xs.at[k], xr.at[k], source,
        )

    s_own = s_ring(h, 0, s.at[pl.ds(h * 64, 64)])
    n_own = wide_ring(nx, h, 1, n.at[h])
    s_other = s_ring(1 - h, 2)
    n_other = wide_ring(nx, 1 - h, 3)
    s_own.start()
    n_own.start()

    for copy in fetch[:6]:
        copy.wait()

    def y_send(b):
        out = []
        for k in kinds:
            for d, to in ((0, 1), (1, 3)):
                ref = blocks[k](b, y)
                out.append(remote(ref, ref, ys.at[k, d], yr.at[k, d], along_y(lax.rem(y + to, 4))))
        for copy in out:
            copy.start()

    def z_copy(k, d, step, b):
        ref = blocks[k](b, y)
        return remote(ref, ref, zs.at[k, d, step], zr.at[k, d, step], along_z(1 - 2 * d))

    lasts = (8, 7)
    sent = []
    for d in (0, 1):
        for k in kinds:
            copy = z_copy(k, d, 0, own)
            copy.start()
            sent.append(copy)
    y_send(own)

    to_far = [
        remote(q.at[0:64], qd.at[h], qs.at[0], qr.at[0, h], (y, 4 + x, before)),
        remote(g.at[0:64], gd.at[h], qs.at[1], qr.at[1, h], (y, 4 + x, before)),
    ]
    to_near = [
        remote(q.at[64:128], qd.at[1], qs.at[2], qr.at[0, 1], partner),
        remote(g.at[64:128], gd.at[1], qs.at[3], qr.at[1, 1], partner),
    ]

    for step in range(1, 9):
        for d in (0, 1):
            if step > lasts[d]:
                continue
            b = z_of(-step if d == 0 else step)
            for k in kinds:
                z_copy(k, d, step - 1, b).wait_recv()
                if step < lasts[d]:
                    copy = z_copy(k, d, step, b)
                    copy.start()
                    sent.append(copy)
            y_send(b)
        if step == 2:
            s_own.middle()
            n_own.middle()
        if step == 4:
            for copy in to_far:
                copy.start()

            @pl.when(h == 1)
            def _():
                for copy in to_near:
                    copy.start()

        if step == 5:
            for copy in swaps:
                copy.wait_recv()
            s_other.start()
            n_other.start()
        if step == 7:
            s_other.middle()
            n_other.middle()

    left, right, far = lax.rem(y + 3, 4), lax.rem(y + 1, 4), lax.rem(y + 2, 4)

    def d_copy(k, i, yy, cc):
        ref = whole[k](yy, cc)
        return remote(ref, ref, ds.at[k, i], dr.at[k, i], sibling)

    for k in kinds:
        d_copy(k, 0, y, c).start()
    for k in kinds:
        for d, yy in ((0, left), (1, right)):
            ref = whole[k](yy, c)
            remote(ref, ref, ys.at[k, d], yr.at[k, d], along_y(right)).wait_recv()
            to = halves[k](yy, d)
            remote(to, to, ys.at[k, 2 + d], yr.at[k, 2 + d], along_y(right if d == 0 else left)).start()
            d_copy(k, 1 + d, yy, c).start()

    def y_finish(k):
        for d in (0, 1):
            to = halves[k](far, d)
            remote(to, to, ys.at[k, 2 + d], yr.at[k, 2 + d], along_y(right)).wait_recv()
        d_copy(k, 3, far, c).start()

    def d_finish(k):
        for i, yy in enumerate((y, left, right, far)):
            d_copy(k, i, yy, 1 - c).wait_recv()

    y_finish(0)
    y_finish(1)
    for copy in fetch[6:]:
        copy.wait()
    for ring in (s_own, n_own, s_other, n_other):
        ring.finish()
    d_finish(0)
    d_finish(1)

    first = lax.broadcasted_iota(jnp.int32, (64, 128), 1) < 64
    mix_rings = []
    for hh in (0, 1):
        total = jnp.zeros((64, 256), F32)
        for tt in range(8):
            total = total + dot(sx[tt], we[hh, tt].reshape(1024, 256))
        both = total.astype(BF)
        key, value = both[:, :128], both[:, 128:]
        query = dot(nx[...], wqo[hh, :, :, :, :, 0:128].reshape(1024, 128)).astype(BF)
        mixed = jnp.zeros((256, 128), F32)
        zero = jnp.zeros((64, 128), BF)
        for keep in (first, jnp.logical_not(first)):
            score = dot(query, jnp.where(keep, key, zero), NT) * (1.0 / math.sqrt(64))
            score = jnp.exp(score - jnp.max(score, axis=-1, keepdims=True))
            weight = (score / jnp.sum(score, axis=-1, keepdims=True)).astype(BF)
            mixed = mixed + dot(weight, jnp.where(keep, value, zero))
        mix[:, lanes(hh * 4 + x, 128)] = mixed.astype(BF)
        ring = wide_ring(mix, hh, 4 + hh)
        ring.start()
        mix_rings.append(ring)
    for ring in mix_rings:
        ring.middle()
    for ring in mix_rings:
        ring.finish()
    prev_rings = []
    for hh in (0, 1):
        at = lanes(hh * 4 + x, 128)
        out = dot(mix[...], wqo[hh, :, :, :, :, 128:256].reshape(1024, 128))
        prev[:, at] = (nx[:, at].astype(F32) + out).astype(BF)
        ring = wide_ring(prev, hh, 6 + hh)
        ring.start()
        prev_rings.append(ring)
    y_finish(2)
    for ring in prev_rings:
        ring.middle()
    for ring in prev_rings:
        ring.finish()
    d_finish(2)

    def q_wait(slot):
        remote(q.at[0:64], qd.at[slot], qs.at[0], qr.at[0, slot], partner).wait_recv()
        remote(g.at[0:64], gd.at[slot], qs.at[1], qr.at[1, slot], partner).wait_recv()

    @pl.when(h == 0)
    def _():
        for copy in home:
            copy.wait()

    @pl.when(h == 1)
    def _():
        q_wait(0)

    q_wait(1)

    token = lax.rem(e * 2 + h + 1, 32) * 64
    position = token + lax.broadcasted_iota(jnp.int32, (64, 128), 0)
    live = jnp.logical_and(position < lens[0], position >= 64)
    scale = 1.0 / math.sqrt(128)

    def heads(turn, carry):
        hh, base = lax.div(turn, 2), lax.rem(turn, 2) * 512
        source = prev[...]
        at_key = pl.ds(pl.multiple_of(base, 512), 512)
        at_value = pl.ds(pl.multiple_of(1024 + base, 512), 512)
        keys = dot(source, wd[hh, :, :, :, :, at_key].reshape(1024, 512)).astype(BF)
        values = dot(source, wd[hh, :, :, :, :, at_value].reshape(1024, 512)).astype(BF)
        for a in range(4):
            at = pl.ds(pl.multiple_of(base + a * 128, 128), 128)
            later = pl.ds(pl.multiple_of(1024 + base + a * 128, 128), 128)
            key, value = keys[:, a * 128 : a * 128 + 128], values[:, a * 128 : a * 128 + 128]
            query = qd[hh, :, at]
            score = dot(query, key, NT) * scale
            score = jnp.exp(score - jnp.max(score, axis=-1, keepdims=True))
            probs = score / jnp.sum(score, axis=-1, keepdims=True)
            low = probs.astype(BF)
            att[hh, :, at] = jnp.where(live, dot(low, value), 0.0).astype(BF)
            cot = jnp.where(live, gd[hh, :, at].astype(F32), 0.0).astype(BF)
            gkv[hh, :, later] = dot(low, cot, TN).astype(BF)
            slope = dot(cot, value, NT)
            inner = jnp.sum(slope * probs, axis=-1, keepdims=True)
            slope = (probs * (slope - inner) * scale).astype(BF)
            gkv[hh, :, at] = dot(slope, query, TN).astype(BF)
        return carry

    lax.fori_loop(0, 4, heads, 0)

    low_rows, high_rows = pl.ds(0, 64), pl.ds(64, 64)
    near = remote(att.at[1], att_out.at[high_rows], as_.at[1], ar.at[1], partner)
    onward = [
        remote(att.at[k], att_out.at[low_rows], as_.at[k], ar.at[0], (y, k * 4 + x, after))
        for k in (0, 1)
    ]

    @pl.when(h == 0)
    def _():
        near.start()
        att_out[64:128, :] = att[0]

    @pl.when(h == 1)
    def _():
        for copy in onward:
            copy.start()

    def share(to):
        total = jnp.zeros((256, 256), F32)
        for hh in (0, 1):
            rows = [
                wd[hh, lax.div(k * 4 + to, 2), pl.ds(lax.rem(to, 2) * 4, 4)].reshape(128, 2048)
                for k in (0, 1)
            ]
            total = total + dot(gkv[hh], jnp.concatenate(rows, axis=0), NT)
        return total

    shares = []
    for k in (2, 1, 3):
        to = lax.rem(x + k, 4)
        part[k - 1] = share(to).astype(BF)
        copy = remote(part.at[k - 1], precv.at[k - 1], rs.at[k - 1], rr.at[k - 1], along_x(to))
        copy.start()
        shares.append(copy)
    total = share(x)
    for k in (1, 3, 2):
        remote(part.at[k - 1], precv.at[k - 1], rs.at[k - 1], rr.at[k - 1], partner).wait_recv()
        total = total + precv[k - 1].astype(F32)
    mine = jnp.where(h == 0, total[:, :128], total[:, 128:])
    other = jnp.where(h == 0, total[:, 128:], total[:, :128])
    gsend[...] = other.astype(BF)
    give = remote(gsend, grecv, hs.at[2], hr.at[2], partner)
    give.start()
    grad_out[h] = mine

    for copy in sent + swaps + to_far + shares:
        copy.wait_send()
    for ring in [s_own, n_own, s_other, n_other] + mix_rings + prev_rings:
        ring.drain()
    for k in kinds:
        for d in (0, 1):
            ref = whole[k](y, c)
            remote(ref, ref, ys.at[k, d], yr.at[k, d], along_y(right)).wait_send()
            to = halves[k](far, d)
            remote(to, to, ys.at[k, 2 + d], yr.at[k, 2 + d], along_y(right)).wait_send()
        for i in range(4):
            d_copy(k, i, y, c).wait_send()

    @pl.when(h == 0)
    def _():
        near.wait_send()

    @pl.when(h == 1)
    def _():
        for copy in to_near + onward:
            copy.wait_send()
        remote(att.at[0], att_out.at[high_rows], as_.at[1], ar.at[1], partner).wait_recv()

    remote(att.at[0], att_out.at[low_rows], as_.at[0], ar.at[0], partner).wait_recv()
    give.wait()
    grad_out[1 - h] = grecv[...].astype(F32)


def on_device(span_states, neighbours, lengths, wq, wk, wv, wo, wkd, wvd, queries, grad_out):
    dma = pltpu.SemaphoreType.DMA
    hbm = pl.BlockSpec(memory_space=pltpu.HBM)
    vmem = pl.BlockSpec(memory_space=pltpu.VMEM)
    return pl.pallas_call(
        kernel,
        out_shape=(
            jax.ShapeDtypeStruct((128, 1024), BF),
            jax.ShapeDtypeStruct((2, 256, 128), F32),
        ),
        in_specs=[pl.BlockSpec(memory_space=pltpu.SMEM)] + [hbm] * 10,
        out_specs=(vmem, vmem),
        scratch_shapes=[
            pltpu.VMEM((2, 8, 2, 4, 128, 256), BF),
            pltpu.VMEM((2, 8, 2, 4, 16, 256), BF),
            pltpu.VMEM((2, 4, 8, 2, 16, 2048), BF),
            pltpu.VMEM((8, 64, 1024), BF),
            pltpu.VMEM((256, 1024), BF),
            pltpu.VMEM((2, 64, 1024), BF),
            pltpu.VMEM((2, 64, 1024), BF),
            pltpu.VMEM((256, 1024), BF),
            pltpu.VMEM((256, 1024), BF),
            pltpu.VMEM((2, 256, 2048), BF),
            pltpu.VMEM((2, 64, 1024), BF),
            pltpu.VMEM((3, 256, 256), BF),
            pltpu.VMEM((3, 256, 256), BF),
            pltpu.VMEM((256, 128), BF),
            pltpu.VMEM((256, 128), BF),
            dma((10,)),
            dma((3, 2, 8)),
            dma((3, 2, 8)),
            dma((3, 4)),
            dma((3, 4)),
            dma((3, 4)),
            dma((3, 4)),
            dma((8, 4)),
            dma((8, 4)),
            dma((3,)),
            dma((3,)),
            dma((4,)),
            dma((2, 2)),
            dma((3,)),
            dma((3,)),
            dma((2,)),
            dma((2,)),
        ],
        compiler_params=pltpu.CompilerParams(
            collective_id=0, has_side_effects=True, vmem_limit_bytes=58 * 1024 * 1024
        ),
    )(lengths, span_states, neighbours, queries, grad_out, wk, wv, wq, wo, wkd, wvd)


def solution(mesh):
    rows = P(("dp", "enc"), "tensor")
    spans = P(("dp", "enc"), None, "tensor")
    weight = P("enc", "tensor")
    return jax.shard_map(
        on_device,
        mesh=mesh,
        in_specs=(rows, spans, P("dp"), weight, weight, weight, weight, rows, rows, rows, rows),
        out_specs=(rows, spans),
        check_vma=False,
    )
```

```python
import math

import jax
import jax.numpy as jnp
from jax import lax
from jax.experimental import pallas as pl
from jax.experimental.pallas import tpu as pltpu
from jax.sharding import PartitionSpec as P

MESH = pl.DeviceIdType.MESH
BF = jnp.bfloat16
F32 = jnp.float32
NT = (((1,), (1,)), ((), ()))
TN = (((0,), (0,)), ((), ()))
NN = (((1,), (0,)), ((), ()))


def dot(a, b, dims=NN):
    return lax.dot_general(a, b, dims, preferred_element_type=F32)


def remote(src, dst, send, recv, device):
    return pltpu.make_async_remote_copy(
        src_ref=src, dst_ref=dst, send_sem=send, recv_sem=recv, device_id=device, device_id_type=MESH
    )


class Ring4:
    def __init__(self, me, device, full, half, send, recv, source=None):
        left, right, far = lax.rem(me + 3, 4), lax.rem(me + 1, 4), lax.rem(me + 2, 4)
        source = full(me) if source is None else source
        self.first = [
            remote(source, full(me), send.at[0], recv.at[0], device(right)),
            remote(source, full(me), send.at[1], recv.at[1], device(left)),
        ]
        self.arrive = [
            remote(full(left), full(left), send.at[0], recv.at[0], device(right)),
            remote(full(right), full(right), send.at[1], recv.at[1], device(left)),
        ]
        self.second = [
            remote(half(left, 0), half(left, 0), send.at[2], recv.at[2], device(right)),
            remote(half(right, 1), half(right, 1), send.at[3], recv.at[3], device(left)),
        ]
        self.last = [
            remote(half(far, 0), half(far, 0), send.at[2], recv.at[2], device(right)),
            remote(half(far, 1), half(far, 1), send.at[3], recv.at[3], device(left)),
        ]

    def start(self):
        for copy in self.first:
            copy.start()

    def middle(self):
        for k in range(2):
            self.arrive[k].wait_recv()
            self.second[k].start()

    def finish(self):
        for copy in self.last:
            copy.wait_recv()

    def drain(self):
        for copy in self.first + self.second:
            copy.wait_send()


def kernel(
    lens, s, n, q, g, wk, wv, wq, wo, wkd, wvd,
    att_out, grad_out,
    we, wqo, wd, sx, nx, qd, gd, kvp, kvs, kvr, mix, prev, gkv, att, part, precv, gsend, grecv,
    n_pass, kv_pass, qg_pass, att_pass, g_pass,
    lsem, zs, zr, ys, yr, ds, dr, xs, xr, hs, hr, qs, qr, rs, rr, as_, ar,
):
    y, t, e = lax.axis_index("dp"), lax.axis_index("tensor"), lax.axis_index("enc")
    h, x = lax.div(t, 4), lax.rem(t, 4)
    j, c = lax.div(e, 2), lax.rem(e, 2)
    z = h * 8 + j
    way = 1 - 2 * c
    before, after = lax.rem(e + 15, 16), lax.rem(e + 1, 16)
    sibling = (y, t, j * 2 + 1 - c)
    near_rows = pl.ds(pl.multiple_of(h * 64, 64), 64)
    far_rows = pl.ds(pl.multiple_of((1 - h) * 64, 64), 64)

    def along_x(i):
        return (y, h * 4 + i, e)

    def along_y(i):
        return (i, t, e)

    def z_of(k):
        zz = lax.rem(z + k + 16, 16)
        return lax.div(zz, 8), lax.rem(zz, 8)

    def along_z(k, core=c):
        hz, jz = z_of(k)
        return (y, hz * 4 + x, jz * 2 + core)

    def lanes(i, width):
        return pl.ds(pl.multiple_of(i * width, width), width)

    next_chip = along_z(way)
    onto = along_z(8 - way)
    from_h, from_j = z_of(-way)
    from_e = from_j * 2 + c

    use = pl.ds(h * 4, 4)
    blocks = (
        lambda b, yy: we.at[b[0], b[1], c, yy],
        lambda b, yy: wqo.at[b[0], b[1], c, yy],
        lambda b, yy: wd.at[b[0], yy, b[1], c],
    )
    whole = (
        lambda yy, cc: we.at[:, use, cc, yy],
        lambda yy, cc: wqo.at[:, :, cc, yy],
        lambda yy, cc: wd.at[:, yy, :, cc],
    )
    halves = (
        lambda yy, k: we.at[k, use, c, yy],
        lambda yy, k: wqo.at[k, :, c, yy],
        lambda yy, k: wd.at[k, yy, :, c],
    )
    kinds = range(3)
    own = (h, j)

    fetch = []

    def local(src, dst):
        copy = pltpu.make_async_copy(src, dst, lsem.at[len(fetch)])
        copy.start()
        fetch.append(copy)

    local(wk.at[pl.ds(y * 128, 128)], we.at[h, j, c, y, :, 0:128])
    local(wv.at[pl.ds(y * 128, 128)], we.at[h, j, c, y, :, 128:256])
    local(wq.at[pl.ds(y * 16, 16)], wqo.at[h, j, c, y, :, 0:128])
    local(wo.at[pl.ds(y * 16, 16)], wqo.at[h, j, c, y, :, 128:256])
    local(wkd, wd.at[h, y, j, c, :, 0:1024])
    local(wvd, wd.at[h, y, j, c, :, 1024:2048])
    local(s, sx.at[x])
    local(n.at[h], nx.at[:, lanes(t, 128)])

    home = [
        pltpu.make_async_copy(q.at[64:128], qd.at[0], lsem.at[8]),
        pltpu.make_async_copy(g.at[64:128], gd.at[0], lsem.at[9]),
    ]

    @pl.when(h == 0)
    def _():
        for copy in home:
            copy.start()

    barrier = pltpu.get_barrier_semaphore()

    def greet(device):
        pl.semaphore_signal(barrier, inc=1, device_id=device, device_id_type=MESH)

    for k in (7, -7):
        greet(along_z(k))
        greet(along_z(k, 1 - c))
    greet((y, 4 + x, before))

    @pl.when(h == 1)
    def _():
        greet((y, x, after))
        greet((y, 4 + x, after))

    for k in (2, 1, 3):
        greet(along_x(lax.rem(x + k, 4)))
    for k in (1, 3):
        greet(along_y(lax.rem(y + k, 4)))
    for k in (1, -1):
        greet(along_z(k))
    greet(sibling)
    pl.semaphore_wait(barrier, 13 + 2 * h)

    def pass_on(k, src, room, dst):
        return (
            remote(src, room, hs.at[0, k], hr.at[0, k], next_chip),
            remote(room, dst, hs.at[1, k], hr.at[1, k], onto),
        )

    n_swap = pass_on(0, n.at[1 - h], n_pass, nx.at[:, lanes(from_h * 4 + x, 128)])
    n_swap[0].start()

    def wide_ring(ref, half_of, k, source=None):
        return Ring4(
            x, along_x,
            lambda i: ref.at[:, lanes(half_of * 4 + i, 128)],
            lambda i, m: ref.at[m * 128 : m * 128 + 128, lanes(half_of * 4 + i, 128)],
            xs.at[k], xr.at[k], source,
        )

    s_ring = Ring4(
        x, along_x, lambda i: sx.at[i], lambda i, m: sx.at[i, m * 64 : m * 64 + 64], xs.at[0], xr.at[0], s
    )
    n_own = wide_ring(nx, h, 1, n.at[h])
    n_other = wide_ring(nx, 1 - h, 2)
    n_own.start()
    s_ring.start()

    for copy in fetch[:6]:
        copy.wait()

    def y_send(b):
        def to_both(k):
            for d, to in ((0, 1), (1, 3)):
                ref = blocks[k](b, y)
                remote(ref, ref, ys.at[k, d], yr.at[k, d], along_y(lax.rem(y + to, 4))).start()

        @pl.when(lax.div(b[1], 4) == h)
        def _():
            to_both(0)

        to_both(1)
        to_both(2)

    def z_copy(k, d, step, b):
        ref = blocks[k](b, y)
        return remote(ref, ref, zs.at[k, d, step], zr.at[k, d, step], along_z(1 - 2 * d))

    lasts = (8, 7)
    sent = []
    for d in (0, 1):
        for k in kinds:
            copy = z_copy(k, d, 0, own)
            copy.start()
            sent.append(copy)
    y_send(own)

    for step in range(1, 9):
        for d in (0, 1):
            if step > lasts[d]:
                continue
            b = z_of(-step if d == 0 else step)
            for k in kinds:
                z_copy(k, d, step - 1, b).wait_recv()
                if step < lasts[d]:
                    copy = z_copy(k, d, step, b)
                    copy.start()
                    sent.append(copy)
            y_send(b)
        if step == 1:
            n_swap[0].wait_recv()
            n_swap[1].start()
            n_own.middle()
        if step == 3:
            s_ring.middle()
        if step == 6:
            n_swap[1].wait_recv()
            n_other.start()

    left, right, far = lax.rem(y + 3, 4), lax.rem(y + 1, 4), lax.rem(y + 2, 4)

    def d_copy(k, i, yy, cc):
        ref = whole[k](yy, cc)
        return remote(ref, ref, ds.at[k, i], dr.at[k, i], sibling)

    def y_middle(k):
        for d, yy in ((0, left), (1, right)):
            ref = whole[k](yy, c)
            remote(ref, ref, ys.at[k, d], yr.at[k, d], along_y(right)).wait_recv()
            to = halves[k](yy, d)
            remote(to, to, ys.at[k, 2 + d], yr.at[k, 2 + d], along_y(right if d == 0 else left)).start()
            d_copy(k, 1 + d, yy, c).start()

    def y_finish(k):
        for d in (0, 1):
            to = halves[k](far, d)
            remote(to, to, ys.at[k, 2 + d], yr.at[k, 2 + d], along_y(right)).wait_recv()
        d_copy(k, 3, far, c).start()

    def d_finish(k):
        for i, yy in enumerate((y, left, right, far)):
            d_copy(k, i, yy, 1 - c).wait_recv()

    for k in kinds:
        d_copy(k, 0, y, c).start()
    for k in kinds:
        y_middle(k)

    q_to, q_from = [], []
    for k, (ref, there) in enumerate(((q, qd), (g, gd))):
        q_to.append((
            remote(ref.at[near_rows], qg_pass.at[k], qs.at[0, k], qr.at[0, k], next_chip),
            remote(ref.at[0:64], there.at[h], qs.at[1, k], qr.at[1 + h, k], (y, 4 + x, before)),
        ))
        q_from.append(
            remote(
                qg_pass.at[k], there.at[from_h], qs.at[2, k], qr.at[1 + from_h, k],
                (y, (1 - from_h) * 4 + x, lax.rem(from_e + 15 + from_h, 16)),
            )
        )
    sends_far = jnp.logical_or(h == 1, c == 1)
    sends_direct = jnp.logical_or(h == 1, c == 0)
    passes_q = jnp.logical_or(from_h == 1, c == 1)

    y_finish(0)
    y_finish(1)
    n_other.middle()
    for copy in fetch[6:]:
        copy.wait()
    for ring in (s_ring, n_own):
        ring.finish()
    d_finish(0)

    for hh in (0, 1):
        total = jnp.zeros((128, 256), F32)
        for i in range(4):
            total = total + dot(sx[i], we[hh, h * 4 + i].reshape(1024, 256))
        kvp[hh] = total
        kvs[hh] = kvp[hh, far_rows].astype(BF)
    kv_swap = pass_on(1, kvs, kv_pass, kvr)
    kv_swap[0].start()
    n_other.finish()
    d_finish(1)
    kv_swap[0].wait_recv()
    kv_swap[1].start()

    @pl.when(sends_far)
    def _():
        for pair in q_to:
            pair[0].start()

    @pl.when(sends_direct)
    def _():
        for pair in q_to:
            pair[1].start()

    queries = []
    for hh in (0, 1):
        queries.append(dot(nx[...], wqo[hh, :, :, :, :, 0:128].reshape(1024, 128)).astype(BF))

    @pl.when(passes_q)
    def _():
        for k in (0, 1):
            q_to[k][0].wait_recv()
            q_from[k].start()

    kv_swap[1].wait_recv()
    first = lax.broadcasted_iota(jnp.int32, (64, 128), 1) < 64
    mix_rings = []
    for hh in (0, 1):
        both = (kvp[hh, near_rows] + kvr[hh].astype(F32)).astype(BF)
        key, value = both[:, :128], both[:, 128:]
        mixed = jnp.zeros((256, 128), F32)
        zero = jnp.zeros((64, 128), BF)
        for keep in (first, jnp.logical_not(first)):
            score = dot(queries[hh], jnp.where(keep, key, zero), NT) * (1.0 / math.sqrt(64))
            score = jnp.exp(score - jnp.max(score, axis=-1, keepdims=True))
            weight = (score / jnp.sum(score, axis=-1, keepdims=True)).astype(BF)
            mixed = mixed + dot(weight, jnp.where(keep, value, zero))
        mix[:, lanes(hh * 4 + x, 128)] = mixed.astype(BF)
        ring = wide_ring(mix, hh, 3 + hh)
        ring.start()
        mix_rings.append(ring)
    for ring in mix_rings:
        ring.middle()
    y_finish(2)
    for ring in mix_rings:
        ring.finish()
    prev_rings = []
    for hh in (0, 1):
        at = lanes(hh * 4 + x, 128)
        out = dot(mix[...], wqo[hh, :, :, :, :, 128:256].reshape(1024, 128))
        prev[:, at] = (nx[:, at].astype(F32) + out).astype(BF)
        ring = wide_ring(prev, hh, 5 + hh)
        ring.start()
        prev_rings.append(ring)
    for ring in prev_rings:
        ring.middle()
    for ring in prev_rings:
        ring.finish()
    d_finish(2)

    def q_wait(slot):
        for k, (ref, there) in enumerate(((q, qd), (g, gd))):
            remote(ref.at[0:64], there.at[slot], qs.at[1, k], qr.at[1 + slot, k], next_chip).wait_recv()

    @pl.when(h == 0)
    def _():
        for copy in home:
            copy.wait()

    @pl.when(h == 1)
    def _():
        q_wait(0)

    q_wait(1)

    token = lax.rem(e * 2 + h + 1, 32) * 64
    position = token + lax.broadcasted_iota(jnp.int32, (64, 128), 0)
    live = jnp.logical_and(position < lens[0], position >= 64)
    scale = 1.0 / math.sqrt(128)

    def heads(turn, carry):
        hh, base = lax.rem(1 - h + lax.div(turn, 2), 2), lax.rem(turn, 2) * 512
        source = prev[...]
        at_key = pl.ds(pl.multiple_of(base, 512), 512)
        at_value = pl.ds(pl.multiple_of(1024 + base, 512), 512)
        keys = dot(source, wd[hh, :, :, :, :, at_key].reshape(1024, 512)).astype(BF)
        values = dot(source, wd[hh, :, :, :, :, at_value].reshape(1024, 512)).astype(BF)
        for a in range(4):
            at = pl.ds(pl.multiple_of(base + a * 128, 128), 128)
            later = pl.ds(pl.multiple_of(1024 + base + a * 128, 128), 128)
            key, value = keys[:, a * 128 : a * 128 + 128], values[:, a * 128 : a * 128 + 128]
            query = qd[hh, :, at]
            score = dot(query, key, NT) * scale
            score = jnp.exp(score - jnp.max(score, axis=-1, keepdims=True))
            probs = score / jnp.sum(score, axis=-1, keepdims=True)
            low = probs.astype(BF)
            att[hh, :, at] = jnp.where(live, dot(low, value), 0.0).astype(BF)
            cot = jnp.where(live, gd[hh, :, at].astype(F32), 0.0).astype(BF)
            gkv[hh, :, later] = dot(low, cot, TN).astype(BF)
            slope = dot(cot, value, NT)
            inner = jnp.sum(slope * probs, axis=-1, keepdims=True)
            slope = (probs * (slope - inner) * scale).astype(BF)
            gkv[hh, :, at] = dot(slope, query, TN).astype(BF)
        return carry

    lax.fori_loop(0, 2, heads, 0)

    low_rows = pl.ds(0, 64)
    att_far = remote(att.at[1 - h], att_pass, as_.at[0], ar.at[2], next_chip)
    att_direct = remote(att.at[0], att_out.at[low_rows], as_.at[0], ar.at[0], (y, x, after))
    att_near = remote(att.at[1], att_out.at[low_rows], as_.at[1], ar.at[0], (y, 4 + x, after))
    att_on = remote(
        att_pass, att_out.at[pl.ds(pl.multiple_of((1 - from_h) * 64, 64), 64)], as_.at[2], ar.at[1 - from_h],
        (y, (1 - from_h) * 4 + x, lax.rem(from_e + from_h, 16)),
    )
    direct = jnp.logical_and(h == 1, c == 1)
    passes_att = jnp.logical_or(from_h == 0, c == 0)

    @pl.when(direct)
    def _():
        att_direct.start()

    @pl.when(jnp.logical_not(direct))
    def _():
        att_far.start()

    lax.fori_loop(2, 4, heads, 0)

    @pl.when(passes_att)
    def _():
        att_far.wait_recv()
        att_on.start()

    @pl.when(h == 0)
    def _():
        att_out[64:128, :] = att[0]

    @pl.when(h == 1)
    def _():
        att_near.start()

    def share(k, to):
        total = jnp.zeros((256, 128), F32)
        for hh in (0, 1):
            rows = wd[hh, lax.div(k * 4 + to, 2), pl.ds(lax.rem(to, 2) * 4, 4)].reshape(128, 2048)
            total = total + dot(gkv[hh], rows, NT)
        return total

    shares = []

    def give_shares(i, k):
        for m in (2, 1, 3):
            to = lax.rem(x + m, 4)
            part[i, m - 1] = share(k, to).astype(BF)
            copy = remote(part.at[i, m - 1], precv.at[i, m - 1], rs.at[i, m - 1], rr.at[i, m - 1], along_x(to))
            copy.start()
            shares.append(copy)

    def take_shares(i, total):
        for m in (1, 3, 2):
            remote(
                part.at[i, m - 1], precv.at[i, m - 1], rs.at[i, m - 1], rr.at[i, m - 1], next_chip
            ).wait_recv()
            total = total + precv[i, m - 1].astype(F32)
        return total

    give_shares(0, 1 - h)
    total = share(1 - h, x)
    gsend[...] = take_shares(0, total).astype(BF)
    g_swap = pass_on(2, gsend, g_pass, grecv)
    g_swap[0].start()
    give_shares(1, h)
    g_swap[0].wait_recv()
    g_swap[1].start()
    grad_out[h] = take_shares(1, share(h, x))

    for copy in sent + shares:
        copy.wait_send()
    for pair in (n_swap, kv_swap, g_swap):
        for copy in pair:
            copy.wait_send()
    for ring in [s_ring, n_own, n_other] + mix_rings + prev_rings:
        ring.drain()
    for k in kinds:
        for d in (0, 1):
            ref = whole[k](y, c)
            remote(ref, ref, ys.at[k, d], yr.at[k, d], along_y(right)).wait_send()
            to = halves[k](far, d)
            remote(to, to, ys.at[k, 2 + d], yr.at[k, 2 + d], along_y(right)).wait_send()
        for i in range(4):
            d_copy(k, i, y, c).wait_send()

    @pl.when(sends_far)
    def _():
        for pair in q_to:
            pair[0].wait_send()

    @pl.when(sends_direct)
    def _():
        for pair in q_to:
            pair[1].wait_send()

    @pl.when(passes_q)
    def _():
        for copy in q_from:
            copy.wait_send()

    @pl.when(direct)
    def _():
        att_direct.wait_send()

    @pl.when(jnp.logical_not(direct))
    def _():
        att_far.wait_send()

    @pl.when(passes_att)
    def _():
        att_on.wait_send()

    @pl.when(h == 1)
    def _():
        att_near.wait_send()
        remote(att.at[0], att_out.at[64:128], as_.at[0], ar.at[1], next_chip).wait_recv()

    remote(att.at[0], att_out.at[low_rows], as_.at[0], ar.at[0], next_chip).wait_recv()
    g_swap[1].wait_recv()
    grad_out[1 - h] = grecv[...].astype(F32)


def on_device(span_states, neighbours, lengths, wq, wk, wv, wo, wkd, wvd, queries, grad_out):
    dma = pltpu.SemaphoreType.DMA
    hbm = pl.BlockSpec(memory_space=pltpu.HBM)
    vmem = pl.BlockSpec(memory_space=pltpu.VMEM)
    return pl.pallas_call(
        kernel,
        out_shape=(
            jax.ShapeDtypeStruct((128, 1024), BF),
            jax.ShapeDtypeStruct((2, 256, 128), F32),
        ),
        in_specs=[pl.BlockSpec(memory_space=pltpu.SMEM)] + [hbm] * 10,
        out_specs=(vmem, vmem),
        scratch_shapes=[
            pltpu.VMEM((2, 8, 2, 4, 128, 256), BF),
            pltpu.VMEM((2, 8, 2, 4, 16, 256), BF),
            pltpu.VMEM((2, 4, 8, 2, 16, 2048), BF),
            pltpu.VMEM((4, 128, 1024), BF),
            pltpu.VMEM((256, 1024), BF),
            pltpu.VMEM((2, 64, 1024), BF),
            pltpu.VMEM((2, 64, 1024), BF),
            pltpu.VMEM((2, 128, 256), F32),
            pltpu.VMEM((2, 64, 256), BF),
            pltpu.VMEM((2, 64, 256), BF),
            pltpu.VMEM((256, 1024), BF),
            pltpu.VMEM((256, 1024), BF),
            pltpu.VMEM((2, 256, 2048), BF),
            pltpu.VMEM((2, 64, 1024), BF),
            pltpu.VMEM((2, 3, 256, 128), BF),
            pltpu.VMEM((2, 3, 256, 128), BF),
            pltpu.VMEM((256, 128), BF),
            pltpu.VMEM((256, 128), BF),
            pltpu.VMEM((256, 128), BF),
            pltpu.VMEM((2, 64, 256), BF),
            pltpu.VMEM((2, 64, 1024), BF),
            pltpu.VMEM((64, 1024), BF),
            pltpu.VMEM((256, 128), BF),
            dma((10,)),
            dma((3, 2, 8)),
            dma((3, 2, 8)),
            dma((3, 4)),
            dma((3, 4)),
            dma((3, 4)),
            dma((3, 4)),
            dma((7, 4)),
            dma((7, 4)),
            dma((2, 3)),
            dma((2, 3)),
            dma((3, 2)),
            dma((3, 2)),
            dma((2, 3)),
            dma((2, 3)),
            dma((3,)),
            dma((3,)),
        ],
        compiler_params=pltpu.CompilerParams(
            collective_id=0, has_side_effects=True, vmem_limit_bytes=58 * 1024 * 1024
        ),
    )(lengths, span_states, neighbours, queries, grad_out, wk, wv, wq, wo, wkd, wvd)


def solution(mesh):
    rows = P(("dp", "enc"), "tensor")
    spans = P(("dp", "enc"), None, "tensor")
    weight = P("enc", "tensor")
    return jax.shard_map(
        on_device,
        mesh=mesh,
        in_specs=(rows, spans, P("dp"), weight, weight, weight, weight, rows, rows, rows, rows),
        out_specs=(rows, spans),
        check_vma=False,
    )
```

```python
import math

import jax
import jax.numpy as jnp
from jax import lax
from jax.experimental import pallas as pl
from jax.experimental.pallas import tpu as pltpu
from jax.sharding import PartitionSpec as P

MESH = pl.DeviceIdType.MESH
BF = jnp.bfloat16
F32 = jnp.float32
NT = (((1,), (1,)), ((), ()))
TN = (((0,), (0,)), ((), ()))
NN = (((1,), (0,)), ((), ()))


def dot(a, b, dims=NN):
    return lax.dot_general(a, b, dims, preferred_element_type=F32)


def remote(src, dst, send, recv, device):
    return pltpu.make_async_remote_copy(
        src_ref=src, dst_ref=dst, send_sem=send, recv_sem=recv, device_id=device, device_id_type=MESH
    )


class Ring4:
    def __init__(self, me, device, full, half, send, recv, source=None):
        left, right, far = lax.rem(me + 3, 4), lax.rem(me + 1, 4), lax.rem(me + 2, 4)
        source = full(me) if source is None else source
        self.first = [
            remote(source, full(me), send.at[0], recv.at[0], device(right)),
            remote(source, full(me), send.at[1], recv.at[1], device(left)),
        ]
        self.arrive = [
            remote(full(left), full(left), send.at[0], recv.at[0], device(right)),
            remote(full(right), full(right), send.at[1], recv.at[1], device(left)),
        ]
        self.second = [
            remote(half(left, 0), half(left, 0), send.at[2], recv.at[2], device(right)),
            remote(half(right, 1), half(right, 1), send.at[3], recv.at[3], device(left)),
        ]
        self.last = [
            remote(half(far, 0), half(far, 0), send.at[2], recv.at[2], device(right)),
            remote(half(far, 1), half(far, 1), send.at[3], recv.at[3], device(left)),
        ]

    def start(self):
        for copy in self.first:
            copy.start()

    def middle(self):
        for k in range(2):
            self.arrive[k].wait_recv()
            self.second[k].start()

    def finish(self):
        for copy in self.last:
            copy.wait_recv()

    def drain(self):
        for copy in self.first + self.second:
            copy.wait_send()


def kernel(
    lens, s, n, q, g, wk, wv, wq, wo, wkd, wvd,
    att_out, grad_out,
    we, wqo, wd, sx, nx, qd, gd, kvp, kvs, kvr, mix, prev, gkv, att, part, precv, gsend, grecv,
    n_pass, kv_pass, qg_pass, att_pass, g_pass,
    lsem, zs, zr, ys, yr, ds, dr, xs, xr, hs, hr, qs, qr, rs, rr, as_, ar, first_came,
):
    y, t, e = lax.axis_index("dp"), lax.axis_index("tensor"), lax.axis_index("enc")
    h, x = lax.div(t, 4), lax.rem(t, 4)
    j, c = lax.div(e, 2), lax.rem(e, 2)
    z = h * 8 + j
    way = 1 - 2 * c
    before, after = lax.rem(e + 15, 16), lax.rem(e + 1, 16)
    sibling = (y, t, j * 2 + 1 - c)
    near_rows = pl.ds(pl.multiple_of(h * 64, 64), 64)
    far_rows = pl.ds(pl.multiple_of((1 - h) * 64, 64), 64)

    def along_x(i):
        return (y, h * 4 + i, e)

    def along_y(i):
        return (i, t, e)

    def z_of(k):
        zz = lax.rem(z + k + 16, 16)
        return lax.div(zz, 8), lax.rem(zz, 8)

    def along_z(k, core=c):
        hz, jz = z_of(k)
        return (y, hz * 4 + x, jz * 2 + core)

    def lanes(i, width):
        return pl.ds(pl.multiple_of(i * width, width), width)

    next_chip = along_z(way)
    onto = along_z(8 - way)
    from_h, from_j = z_of(-way)
    from_e = from_j * 2 + c

    use = pl.ds(h * 4, 4)
    blocks = (
        lambda b, yy: we.at[b[0], b[1], c, yy],
        lambda b, yy: wqo.at[b[0], b[1], c, yy],
        lambda b, yy: wd.at[b[0], yy, b[1], c],
    )
    whole = (
        lambda yy, cc: we.at[:, use, cc, yy],
        lambda yy, cc: wqo.at[:, :, cc, yy],
        lambda yy, cc: wd.at[:, yy, :, cc],
    )
    halves = (
        lambda yy, k: we.at[k, use, c, yy],
        lambda yy, k: wqo.at[k, :, c, yy],
        lambda yy, k: wd.at[k, yy, :, c],
    )
    kinds = range(3)
    own = (h, j)

    fetch = []

    def local(src, dst):
        copy = pltpu.make_async_copy(src, dst, lsem.at[len(fetch)])
        copy.start()
        fetch.append(copy)

    local(wk.at[pl.ds(y * 128, 128)], we.at[h, j, c, y, :, 0:128])
    local(wv.at[pl.ds(y * 128, 128)], we.at[h, j, c, y, :, 128:256])
    local(wq.at[pl.ds(y * 16, 16)], wqo.at[h, j, c, y, :, 0:128])
    local(wo.at[pl.ds(y * 16, 16)], wqo.at[h, j, c, y, :, 128:256])
    local(wkd, wd.at[h, y, j, c, :, 0:1024])
    local(wvd, wd.at[h, y, j, c, :, 1024:2048])
    local(s, sx.at[x])
    local(n.at[h], nx.at[:, lanes(t, 128)])

    home = [
        pltpu.make_async_copy(q.at[64:128], qd.at[0], lsem.at[8]),
        pltpu.make_async_copy(g.at[64:128], gd.at[0], lsem.at[9]),
    ]

    @pl.when(h == 0)
    def _():
        for copy in home:
            copy.start()

    barrier = pltpu.get_barrier_semaphore()

    def greet(device):
        pl.semaphore_signal(barrier, inc=1, device_id=device, device_id_type=MESH)

    for k in (7, -7):
        greet(along_z(k))
        greet(along_z(k, 1 - c))
    greet((y, 4 + x, before))

    @pl.when(h == 1)
    def _():
        greet((y, x, after))
        greet((y, 4 + x, after))

    for k in (2, 1, 3):
        greet(along_x(lax.rem(x + k, 4)))
    for k in (1, 3):
        greet(along_y(lax.rem(y + k, 4)))
    for k in (5, -5, 1, -1):
        greet(along_z(k))
    greet(sibling)
    pl.semaphore_wait(barrier, 15 + 2 * h)

    def pass_on(k, src, room, dst):
        return (
            remote(src, room, hs.at[0, k], hr.at[0, k], next_chip),
            remote(room, dst, hs.at[1, k], hr.at[1, k], onto),
        )

    n_swap = pass_on(0, n.at[1 - h], n_pass, nx.at[:, lanes(from_h * 4 + x, 128)])
    n_swap[0].start()

    def wide_ring(ref, half_of, k, source=None):
        return Ring4(
            x, along_x,
            lambda i: ref.at[:, lanes(half_of * 4 + i, 128)],
            lambda i, m: ref.at[m * 128 : m * 128 + 128, lanes(half_of * 4 + i, 128)],
            xs.at[k], xr.at[k], source,
        )

    s_ring = Ring4(
        x, along_x, lambda i: sx.at[i], lambda i, m: sx.at[i, m * 64 : m * 64 + 64], xs.at[0], xr.at[0], s
    )
    n_own = wide_ring(nx, h, 1, n.at[h])
    n_other = wide_ring(nx, 1 - h, 2)
    n_own.start()
    s_ring.start()

    for copy in fetch[:6]:
        copy.wait()

    left, right, far = lax.rem(y + 3, 4), lax.rem(y + 1, 4), lax.rem(y + 2, 4)

    def used(b):
        return pl.when(lax.div(b[1], 4) == h)

    def y_copy(k, d, i, b, yy):
        ref = blocks[k](b, yy)
        came = first_came.at[d, i] if k == 0 else yr.at[k, d]
        return remote(ref, ref, ys.at[k, d], came, along_y(right if d == 0 else left))

    def y_send(k, i, b):
        def to_both():
            for d in (0, 1):
                y_copy(k, d, i, b, y).start()

        if k == 0:
            used(b)(to_both)
        else:
            to_both()

    def y_onward(i, b):
        @used(b)
        def _():
            for d, yy in ((0, left), (1, right)):
                y_copy(0, d, i, b, yy).wait_recv()
                ref = blocks[0](b, yy).at[:, d * 128 : d * 128 + 128]
                remote(ref, ref, ys.at[0, 2 + d], yr.at[0, 2 + d], along_y(right if d == 0 else left)).start()

    def d_copy(k, i, yy, cc):
        ref = whole[k](yy, cc)
        return remote(ref, ref, ds.at[k, i], dr.at[k, i], sibling)

    def y_middle(k):
        for d, yy in ((0, left), (1, right)):
            ref = whole[k](yy, c)
            remote(ref, ref, ys.at[k, d], yr.at[k, d], along_y(right)).wait_recv()
            to = halves[k](yy, d)
            remote(to, to, ys.at[k, 2 + d], yr.at[k, 2 + d], along_y(right if d == 0 else left)).start()
            d_copy(k, 1 + d, yy, c).start()

    def y_finish(k):
        for d in (0, 1):
            to = halves[k](far, d)
            remote(to, to, ys.at[k, 2 + d], yr.at[k, 2 + d], along_y(right)).wait_recv()
        d_copy(k, 3, far, c).start()

    def d_finish(k):
        for i, yy in enumerate((y, left, right, far)):
            d_copy(k, i, yy, 1 - c).wait_recv()

    q_to, q_from = [], []
    for k, (ref, there) in enumerate(((q, qd), (g, gd))):
        q_to.append((
            remote(ref.at[near_rows], qg_pass.at[k], qs.at[0, k], qr.at[0, k], next_chip),
            remote(ref.at[0:64], there.at[h], qs.at[1, k], qr.at[1 + h, k], (y, 4 + x, before)),
        ))
        q_from.append(
            remote(
                qg_pass.at[k], there.at[from_h], qs.at[2, k], qr.at[1 + from_h, k],
                (y, (1 - from_h) * 4 + x, lax.rem(from_e + 15 + from_h, 16)),
            )
        )
    sends_far = jnp.logical_or(h == 1, c == 1)
    sends_direct = jnp.logical_or(h == 1, c == 0)
    passes_q = jnp.logical_or(from_h == 1, c == 1)

    def q_start(k):
        @pl.when(sends_far)
        def _():
            q_to[k][0].start()

        @pl.when(sends_direct)
        def _():
            q_to[k][1].start()

    def q_pass(k):
        @pl.when(passes_q)
        def _():
            q_to[k][0].wait_recv()
            q_from[k].start()

    lasts = (8, 7)
    sent = []

    def z_copy(k, d, at, b, hops=1):
        ref = blocks[k](b, y)
        return remote(ref, ref, zs.at[k, d, at - 1], zr.at[k, d, at - 1], along_z(hops - 2 * hops * d))

    def z_start(k, d, at, b, hops=1):
        copy = z_copy(k, d, at, b, hops)
        copy.start()
        sent.append(copy)

    def z_take(k, d, at):
        b = z_of(-at if d == 0 else at)
        z_copy(k, d, at, b).wait_recv()
        if at != lasts[d] and (k == 2 or at != 4):
            z_start(k, d, at + 1, b)
        return d * 8 + at, b

    for k in (0, 1):
        for d in (0, 1):
            z_start(k, d, 1, own)
        for d in (0, 1):
            z_start(k, d, 5, own, 5)
    for d in (0, 1):
        z_start(2, d, 1, own)
    for k in (0, 1):
        y_send(k, 0, own)

    early, late = [(0, own)], [(0, own)]
    for step in range(1, 9):
        came = [(d, at) for at in (step, step + 3) for d in (0, 1) if at <= lasts[d]]
        came = [(d, at) for d, at in came if (at == step and step <= 4) or (at > 4 and at == step + 3)]
        for k in (0, 1):
            for d, at in came:
                i, b = z_take(k, d, at)
                y_send(k, i, b)
                if k == 0:
                    early.append((i, b))
        for d in (0, 1):
            if step <= lasts[d]:
                late.append(z_take(2, d, step))
        if step == 1:
            n_swap[0].wait_recv()
            n_swap[1].start()
            n_own.middle()
        if step >= 2:
            keep = len(came)
            for i, b in early[: len(early) - keep]:
                y_onward(i, b)
            early = early[len(early) - keep :]
        if step == 3:
            s_ring.middle()
        if step == 5:
            q_start(0)
        if step == 6:
            n_swap[1].wait_recv()
            n_other.start()
            q_pass(0)
        if step >= 6:
            for i, b in late:
                y_send(2, i, b)
            late = []
        if step == 6:
            for i, yy in enumerate((y, left, right)):
                d_copy(0, i, yy, c).start()
            d_copy(1, 0, y, c).start()
            y_middle(1)
        if step == 7:
            y_finish(0)

    d_copy(2, 0, y, c).start()
    n_other.middle()
    for copy in fetch[6:]:
        copy.wait()
    for ring in (s_ring, n_own):
        ring.finish()
    y_finish(1)
    d_finish(0)

    for hh in (0, 1):
        total = jnp.zeros((128, 256), F32)
        for i in range(4):
            total = total + dot(sx[i], we[hh, h * 4 + i].reshape(1024, 256))
        kvp[hh] = total
        kvs[hh] = kvp[hh, far_rows].astype(BF)
    kv_swap = pass_on(1, kvs, kv_pass, kvr)
    kv_swap[0].start()
    n_other.finish()
    d_finish(1)
    kv_swap[0].wait_recv()
    kv_swap[1].start()
    q_start(1)
    queries = []
    for hh in (0, 1):
        queries.append(dot(nx[...], wqo[hh, :, :, :, :, 0:128].reshape(1024, 128)).astype(BF))

    q_pass(1)
    y_middle(2)
    kv_swap[1].wait_recv()
    first = lax.broadcasted_iota(jnp.int32, (64, 128), 1) < 64
    mix_rings = []
    for hh in (0, 1):
        both = (kvp[hh, near_rows] + kvr[hh].astype(F32)).astype(BF)
        key, value = both[:, :128], both[:, 128:]
        mixed = jnp.zeros((256, 128), F32)
        zero = jnp.zeros((64, 128), BF)
        for keep in (first, jnp.logical_not(first)):
            score = dot(queries[hh], jnp.where(keep, key, zero), NT) * (1.0 / math.sqrt(64))
            score = jnp.exp(score - jnp.max(score, axis=-1, keepdims=True))
            weight = (score / jnp.sum(score, axis=-1, keepdims=True)).astype(BF)
            mixed = mixed + dot(weight, jnp.where(keep, value, zero))
        mix[:, lanes(hh * 4 + x, 128)] = mixed.astype(BF)
        ring = wide_ring(mix, hh, 3 + hh)
        ring.start()
        mix_rings.append(ring)
    for ring in mix_rings:
        ring.middle()
    y_finish(2)
    for ring in mix_rings:
        ring.finish()
    prev_rings = []
    for hh in (0, 1):
        at = lanes(hh * 4 + x, 128)
        out = dot(mix[...], wqo[hh, :, :, :, :, 128:256].reshape(1024, 128))
        prev[:, at] = (nx[:, at].astype(F32) + out).astype(BF)
        ring = wide_ring(prev, hh, 5 + hh)
        ring.start()
        prev_rings.append(ring)
    for ring in prev_rings:
        ring.middle()
    for ring in prev_rings:
        ring.finish()
    d_finish(2)

    def q_wait(slot):
        for k, (ref, there) in enumerate(((q, qd), (g, gd))):
            remote(ref.at[0:64], there.at[slot], qs.at[1, k], qr.at[1 + slot, k], next_chip).wait_recv()

    @pl.when(h == 0)
    def _():
        for copy in home:
            copy.wait()

    @pl.when(h == 1)
    def _():
        q_wait(0)

    q_wait(1)

    token = lax.rem(e * 2 + h + 1, 32) * 64
    position = token + lax.broadcasted_iota(jnp.int32, (64, 128), 0)
    live = jnp.logical_and(position < lens[0], position >= 64)
    scale = 1.0 / math.sqrt(128)

    def heads(turn):
        hh, base = (1 - h if turn < 2 else h), turn % 2 * 512
        source = prev[...]
        at_key = slice(base, base + 512)
        at_value = slice(1024 + base, 1536 + base)
        keys = dot(source, wd[hh, :, :, :, :, at_key].reshape(1024, 512)).astype(BF)
        values = dot(source, wd[hh, :, :, :, :, at_value].reshape(1024, 512)).astype(BF)
        for a in range(4):
            at = slice(base + a * 128, base + a * 128 + 128)
            later = slice(1024 + base + a * 128, 1152 + base + a * 128)
            key, value = keys[:, a * 128 : a * 128 + 128], values[:, a * 128 : a * 128 + 128]
            query = qd[hh, :, at]
            score = dot(query, key, NT) * scale
            score = jnp.exp(score - jnp.max(score, axis=-1, keepdims=True))
            probs = score / jnp.sum(score, axis=-1, keepdims=True)
            low = probs.astype(BF)
            att[hh, :, at] = jnp.where(live, dot(low, value), 0.0).astype(BF)
            cot = jnp.where(live, gd[hh, :, at].astype(F32), 0.0).astype(BF)
            gkv[hh, :, later] = dot(low, cot, TN).astype(BF)
            slope = dot(cot, value, NT)
            inner = jnp.sum(slope * probs, axis=-1, keepdims=True)
            slope = (probs * (slope - inner) * scale).astype(BF)
            gkv[hh, :, at] = dot(slope, query, TN).astype(BF)

    low_rows = pl.ds(0, 64)
    on_rows = pl.ds(pl.multiple_of((1 - from_h) * 64, 64), 64)
    on_device_id = (y, (1 - from_h) * 4 + x, lax.rem(from_e + from_h, 16))
    att_far, att_direct, att_on = [], [], []
    for k in (0, 1):
        part_of = slice(k * 512, k * 512 + 512)
        att_far.append(
            remote(att.at[1 - h, :, part_of], att_pass.at[:, part_of], as_.at[k], ar.at[2 + k], next_chip)
        )
        att_direct.append(
            remote(att.at[0, :, part_of], att_out.at[low_rows, part_of], as_.at[k], ar.at[0], (y, x, after))
        )
        att_on.append(
            remote(
                att_pass.at[:, part_of], att_out.at[on_rows, part_of], as_.at[2 + k], ar.at[1 - from_h],
                on_device_id,
            )
        )
    att_near = remote(att.at[1], att_out.at[low_rows], as_.at[4], ar.at[0], (y, 4 + x, after))
    direct = jnp.logical_and(h == 1, c == 1)
    passes_att = jnp.logical_or(from_h == 0, c == 0)

    def att_start(k):
        @pl.when(direct)
        def _():
            att_direct[k].start()

        @pl.when(jnp.logical_not(direct))
        def _():
            att_far[k].start()

    def att_pass_on(k):
        @pl.when(passes_att)
        def _():
            att_far[k].wait_recv()
            att_on[k].start()

    heads(0)
    att_start(0)
    heads(1)
    att_start(1)
    att_pass_on(0)
    heads(2)
    att_pass_on(1)
    heads(3)

    @pl.when(h == 0)
    def _():
        att_out[64:128, :] = att[0]

    @pl.when(h == 1)
    def _():
        att_near.start()

    def share(k, to):
        total = jnp.zeros((256, 128), F32)
        for hh in (0, 1):
            rows = wd[hh, lax.div(k * 4 + to, 2), pl.ds(lax.rem(to, 2) * 4, 4)].reshape(128, 2048)
            total = total + dot(gkv[hh], rows, NT)
        return total

    shares = []

    def give_shares(i, k):
        for m in (2, 1, 3):
            to = lax.rem(x + m, 4)
            part[i, m - 1] = share(k, to).astype(BF)
            copy = remote(part.at[i, m - 1], precv.at[i, m - 1], rs.at[i, m - 1], rr.at[i, m - 1], along_x(to))
            copy.start()
            shares.append(copy)

    def take_shares(i, total):
        for m in (1, 3, 2):
            remote(
                part.at[i, m - 1], precv.at[i, m - 1], rs.at[i, m - 1], rr.at[i, m - 1], next_chip
            ).wait_recv()
            total = total + precv[i, m - 1].astype(F32)
        return total

    give_shares(0, 1 - h)
    total = share(1 - h, x)
    gsend[...] = take_shares(0, total).astype(BF)
    g_swap = pass_on(2, gsend, g_pass, grecv)
    g_swap[0].start()
    give_shares(1, h)
    g_swap[0].wait_recv()
    g_swap[1].start()
    grad_out[h] = take_shares(1, share(h, x))

    for copy in sent + shares:
        copy.wait_send()
    for pair in (n_swap, kv_swap, g_swap):
        for copy in pair:
            copy.wait_send()
    for ring in [s_ring, n_own, n_other] + mix_rings + prev_rings:
        ring.drain()
    for k in kinds:
        for d in (0, 1):
            ref = whole[k](y, c)
            remote(ref, ref, ys.at[k, d], yr.at[k, d], along_y(right)).wait_send()
            to = halves[k](far, d)
            remote(to, to, ys.at[k, 2 + d], yr.at[k, 2 + d], along_y(right)).wait_send()
        for i in range(4):
            d_copy(k, i, y, c).wait_send()

    @pl.when(sends_far)
    def _():
        for pair in q_to:
            pair[0].wait_send()

    @pl.when(sends_direct)
    def _():
        for pair in q_to:
            pair[1].wait_send()

    @pl.when(passes_q)
    def _():
        for copy in q_from:
            copy.wait_send()

    @pl.when(direct)
    def _():
        for copy in att_direct:
            copy.wait_send()

    @pl.when(jnp.logical_not(direct))
    def _():
        for copy in att_far:
            copy.wait_send()

    @pl.when(passes_att)
    def _():
        for copy in att_on:
            copy.wait_send()

    @pl.when(h == 1)
    def _():
        att_near.wait_send()
        remote(att.at[0], att_out.at[64:128], as_.at[0], ar.at[1], next_chip).wait_recv()

    remote(att.at[0], att_out.at[low_rows], as_.at[0], ar.at[0], next_chip).wait_recv()
    g_swap[1].wait_recv()
    grad_out[1 - h] = grecv[...].astype(F32)


def on_device(span_states, neighbours, lengths, wq, wk, wv, wo, wkd, wvd, queries, grad_out):
    dma = pltpu.SemaphoreType.DMA
    hbm = pl.BlockSpec(memory_space=pltpu.HBM)
    vmem = pl.BlockSpec(memory_space=pltpu.VMEM)
    return pl.pallas_call(
        kernel,
        out_shape=(
            jax.ShapeDtypeStruct((128, 1024), BF),
            jax.ShapeDtypeStruct((2, 256, 128), F32),
        ),
        in_specs=[pl.BlockSpec(memory_space=pltpu.SMEM)] + [hbm] * 10,
        out_specs=(vmem, vmem),
        scratch_shapes=[
            pltpu.VMEM((2, 8, 2, 4, 128, 256), BF),
            pltpu.VMEM((2, 8, 2, 4, 16, 256), BF),
            pltpu.VMEM((2, 4, 8, 2, 16, 2048), BF),
            pltpu.VMEM((4, 128, 1024), BF),
            pltpu.VMEM((256, 1024), BF),
            pltpu.VMEM((2, 64, 1024), BF),
            pltpu.VMEM((2, 64, 1024), BF),
            pltpu.VMEM((2, 128, 256), F32),
            pltpu.VMEM((2, 64, 256), BF),
            pltpu.VMEM((2, 64, 256), BF),
            pltpu.VMEM((256, 1024), BF),
            pltpu.VMEM((256, 1024), BF),
            pltpu.VMEM((2, 256, 2048), BF),
            pltpu.VMEM((2, 64, 1024), BF),
            pltpu.VMEM((2, 3, 256, 128), BF),
            pltpu.VMEM((2, 3, 256, 128), BF),
            pltpu.VMEM((256, 128), BF),
            pltpu.VMEM((256, 128), BF),
            pltpu.VMEM((256, 128), BF),
            pltpu.VMEM((2, 64, 256), BF),
            pltpu.VMEM((2, 64, 1024), BF),
            pltpu.VMEM((64, 1024), BF),
            pltpu.VMEM((256, 128), BF),
            dma((10,)),
            dma((3, 2, 8)),
            dma((3, 2, 8)),
            dma((3, 4)),
            dma((3, 4)),
            dma((3, 4)),
            dma((3, 4)),
            dma((7, 4)),
            dma((7, 4)),
            dma((2, 3)),
            dma((2, 3)),
            dma((3, 2)),
            dma((3, 2)),
            dma((2, 3)),
            dma((2, 3)),
            dma((5,)),
            dma((4,)),
            dma((2, 16)),
        ],
        compiler_params=pltpu.CompilerParams(
            collective_id=0, has_side_effects=True, vmem_limit_bytes=58 * 1024 * 1024
        ),
    )(lengths, span_states, neighbours, queries, grad_out, wk, wv, wq, wo, wkd, wvd)


def solution(mesh):
    rows = P(("dp", "enc"), "tensor")
    spans = P(("dp", "enc"), None, "tensor")
    weight = P("enc", "tensor")
    return jax.shard_map(
        on_device,
        mesh=mesh,
        in_specs=(rows, spans, P("dp"), weight, weight, weight, weight, rows, rows, rows, rows),
        out_specs=(rows, spans),
        check_vma=False,
    )
```

```python
import math

import jax
import jax.numpy as jnp
from jax import lax
from jax.experimental import pallas as pl
from jax.experimental.pallas import tpu as pltpu
from jax.sharding import PartitionSpec as P

MESH = pl.DeviceIdType.MESH
BF = jnp.bfloat16
F32 = jnp.float32
NT = (((1,), (1,)), ((), ()))
TN = (((0,), (0,)), ((), ()))
NN = (((1,), (0,)), ((), ()))


def dot(a, b, dims=NN):
    return lax.dot_general(a, b, dims, preferred_element_type=F32)


def remote(src, dst, send, recv, device):
    return pltpu.make_async_remote_copy(
        src_ref=src, dst_ref=dst, send_sem=send, recv_sem=recv, device_id=device, device_id_type=MESH
    )


class Ring4:
    def __init__(self, me, device, full, half, send, recv, source=None):
        left, right, far = lax.rem(me + 3, 4), lax.rem(me + 1, 4), lax.rem(me + 2, 4)
        source = full(me) if source is None else source
        self.first = [
            remote(source, full(me), send.at[0], recv.at[0], device(right)),
            remote(source, full(me), send.at[1], recv.at[1], device(left)),
        ]
        self.arrive = [
            remote(full(left), full(left), send.at[0], recv.at[0], device(right)),
            remote(full(right), full(right), send.at[1], recv.at[1], device(left)),
        ]
        self.second = [
            remote(half(left, 0), half(left, 0), send.at[2], recv.at[2], device(right)),
            remote(half(right, 1), half(right, 1), send.at[3], recv.at[3], device(left)),
        ]
        self.last = [
            remote(half(far, 0), half(far, 0), send.at[2], recv.at[2], device(right)),
            remote(half(far, 1), half(far, 1), send.at[3], recv.at[3], device(left)),
        ]

    def start(self):
        for copy in self.first:
            copy.start()

    def middle(self):
        for k in range(2):
            self.arrive[k].wait_recv()
            self.second[k].start()

    def finish(self):
        for copy in self.last:
            copy.wait_recv()

    def drain(self):
        for copy in self.first + self.second:
            copy.wait_send()


def kernel(
    lens, s, n, q, g, wk, wv, wq, wo, wkd, wvd,
    att_out, grad_out,
    we, wqo, wd, sx, nx, qd, gd, kvp, kvs, kvr, mix, prev, gkv, att, part, precv, gsum, gsend, grecv,
    n_pass, kv_pass, qg_pass, att_pass, g_pass,
    lsem, zs, zr, ys, yr, ds, dr, xs, xr, hs, hr, qs, qr, rs, rr, as_, ar, first_came,
):
    y, t, e = lax.axis_index("dp"), lax.axis_index("tensor"), lax.axis_index("enc")
    h, x = lax.div(t, 4), lax.rem(t, 4)
    j, c = lax.div(e, 2), lax.rem(e, 2)
    z = h * 8 + j
    way = 1 - 2 * c
    before, after = lax.rem(e + 15, 16), lax.rem(e + 1, 16)
    sibling = (y, t, j * 2 + 1 - c)
    near_rows = pl.ds(pl.multiple_of(h * 64, 64), 64)
    far_rows = pl.ds(pl.multiple_of((1 - h) * 64, 64), 64)

    def along_x(i):
        return (y, h * 4 + i, e)

    def along_y(i):
        return (i, t, e)

    def z_of(k):
        zz = lax.rem(z + k + 16, 16)
        return lax.div(zz, 8), lax.rem(zz, 8)

    def along_z(k, core=c):
        hz, jz = z_of(k)
        return (y, hz * 4 + x, jz * 2 + core)

    def lanes(i, width):
        return pl.ds(pl.multiple_of(i * width, width), width)

    next_chip = along_z(way)
    onto = along_z(8 - way)
    from_h, from_j = z_of(-way)
    from_e = from_j * 2 + c

    use = pl.ds(h * 4, 4)
    blocks = (
        lambda b, yy: we.at[b[0], b[1], c, yy],
        lambda b, yy: wqo.at[b[0], b[1], c, yy],
        lambda b, yy: wd.at[b[0], yy, b[1], c],
    )
    whole = (
        lambda yy, cc: we.at[:, use, cc, yy],
        lambda yy, cc: wqo.at[:, :, cc, yy],
        lambda yy, cc: wd.at[:, yy, :, cc],
    )
    halves = (
        lambda yy, k: we.at[k, use, c, yy],
        lambda yy, k: wqo.at[k, :, c, yy],
        lambda yy, k: wd.at[k, yy, :, c],
    )
    kinds = range(3)
    own = (h, j)

    fetch = []

    def local(src, dst):
        copy = pltpu.make_async_copy(src, dst, lsem.at[len(fetch)])
        copy.start()
        fetch.append(copy)

    local(wk.at[pl.ds(y * 128, 128)], we.at[h, j, c, y, :, 0:128])
    local(wv.at[pl.ds(y * 128, 128)], we.at[h, j, c, y, :, 128:256])
    local(wq.at[pl.ds(y * 16, 16)], wqo.at[h, j, c, y, :, 0:128])
    local(wo.at[pl.ds(y * 16, 16)], wqo.at[h, j, c, y, :, 128:256])
    local(wkd, wd.at[h, y, j, c, :, 0:1024])
    local(wvd, wd.at[h, y, j, c, :, 1024:2048])
    local(s, sx.at[x])
    local(n.at[h], nx.at[:, lanes(t, 128)])

    home = [
        pltpu.make_async_copy(q.at[64:128], qd.at[0], lsem.at[8]),
        pltpu.make_async_copy(g.at[64:128], gd.at[0], lsem.at[9]),
    ]

    @pl.when(h == 0)
    def _():
        for copy in home:
            copy.start()

    barrier = pltpu.get_barrier_semaphore()

    def greet(device):
        pl.semaphore_signal(barrier, inc=1, device_id=device, device_id_type=MESH)

    for k in (7, -7):
        greet(along_z(k))
        greet(along_z(k, 1 - c))
    greet((y, 4 + x, before))

    @pl.when(h == 1)
    def _():
        greet((y, x, after))
        greet((y, 4 + x, after))

    for k in (2, 1, 3):
        greet(along_x(lax.rem(x + k, 4)))
    for k in (1, 3):
        greet(along_y(lax.rem(y + k, 4)))
    for k in (5, -5, 1, -1):
        greet(along_z(k))
    greet(sibling)
    pl.semaphore_wait(barrier, 15 + 2 * h)

    def pass_on(k, src, room, dst):
        return (
            remote(src, room, hs.at[0, k], hr.at[0, k], next_chip),
            remote(room, dst, hs.at[1, k], hr.at[1, k], onto),
        )

    n_swap = pass_on(0, n.at[1 - h], n_pass, nx.at[:, lanes(from_h * 4 + x, 128)])
    n_swap[0].start()

    def wide_ring(ref, half_of, k, source=None):
        return Ring4(
            x, along_x,
            lambda i: ref.at[:, lanes(half_of * 4 + i, 128)],
            lambda i, m: ref.at[m * 128 : m * 128 + 128, lanes(half_of * 4 + i, 128)],
            xs.at[k], xr.at[k], source,
        )

    s_ring = Ring4(
        x, along_x, lambda i: sx.at[i], lambda i, m: sx.at[i, m * 64 : m * 64 + 64], xs.at[0], xr.at[0], s
    )
    n_own = wide_ring(nx, h, 1, n.at[h])
    n_other = wide_ring(nx, 1 - h, 2)
    n_own.start()
    s_ring.start()

    for copy in fetch[:6]:
        copy.wait()

    left, right, far = lax.rem(y + 3, 4), lax.rem(y + 1, 4), lax.rem(y + 2, 4)

    def used(b):
        return pl.when(lax.div(b[1], 4) == h)

    def y_copy(k, d, i, b, yy):
        ref = blocks[k](b, yy)
        came = first_came.at[d, i] if k == 0 else yr.at[k, d]
        return remote(ref, ref, ys.at[k, d], came, along_y(right if d == 0 else left))

    def y_send(k, i, b):
        def to_both():
            for d in (0, 1):
                y_copy(k, d, i, b, y).start()

        if k == 0:
            used(b)(to_both)
        else:
            to_both()

    def y_onward(i, b):
        @used(b)
        def _():
            for d, yy in ((0, left), (1, right)):
                y_copy(0, d, i, b, yy).wait_recv()
                ref = blocks[0](b, yy).at[:, d * 128 : d * 128 + 128]
                remote(ref, ref, ys.at[0, 2 + d], yr.at[0, 2 + d], along_y(right if d == 0 else left)).start()

    def d_copy(k, i, yy, cc):
        ref = whole[k](yy, cc)
        return remote(ref, ref, ds.at[k, i], dr.at[k, i], sibling)

    def y_middle(k):
        for d, yy in ((0, left), (1, right)):
            ref = whole[k](yy, c)
            remote(ref, ref, ys.at[k, d], yr.at[k, d], along_y(right)).wait_recv()
            to = halves[k](yy, d)
            remote(to, to, ys.at[k, 2 + d], yr.at[k, 2 + d], along_y(right if d == 0 else left)).start()
            d_copy(k, 1 + d, yy, c).start()

    def y_finish(k):
        for d in (0, 1):
            to = halves[k](far, d)
            remote(to, to, ys.at[k, 2 + d], yr.at[k, 2 + d], along_y(right)).wait_recv()
        d_copy(k, 3, far, c).start()

    def d_finish(k):
        for i, yy in enumerate((y, left, right, far)):
            d_copy(k, i, yy, 1 - c).wait_recv()

    q_to, q_from = [], []
    for k, (ref, there) in enumerate(((q, qd), (g, gd))):
        q_to.append((
            remote(ref.at[near_rows], qg_pass.at[k], qs.at[0, k], qr.at[0, k], next_chip),
            remote(ref.at[0:64], there.at[h], qs.at[1, k], qr.at[1 + h, k], (y, 4 + x, before)),
        ))
        q_from.append(
            remote(
                qg_pass.at[k], there.at[from_h], qs.at[2, k], qr.at[1 + from_h, k],
                (y, (1 - from_h) * 4 + x, lax.rem(from_e + 15 + from_h, 16)),
            )
        )
    sends_far = jnp.logical_or(h == 1, c == 1)
    sends_direct = jnp.logical_or(h == 1, c == 0)
    passes_q = jnp.logical_or(from_h == 1, c == 1)

    def q_start(k):
        @pl.when(sends_far)
        def _():
            q_to[k][0].start()

        @pl.when(sends_direct)
        def _():
            q_to[k][1].start()

    def q_pass(k):
        @pl.when(passes_q)
        def _():
            q_to[k][0].wait_recv()
            q_from[k].start()

    lasts = (8, 7)
    sent = []

    def z_copy(k, d, at, b, hops=1):
        ref = blocks[k](b, y)
        return remote(ref, ref, zs.at[k, d, at - 1], zr.at[k, d, at - 1], along_z(hops - 2 * hops * d))

    def wanted(k, d, at, b):
        if k != 0:
            return lambda body: body()
        end = 4 if at <= 4 else lasts[d]
        goal, some = lax.div(b[1], 4), False
        for reach in range(at, end + 1):
            there = lax.rem(b[0] * 8 + b[1] + (reach if d == 0 else 16 - reach), 16)
            some = jnp.logical_or(some, lax.div(there, 8) == goal)
        return pl.when(some)

    def z_start(k, d, at, b, hops=1):
        copy = z_copy(k, d, at, b, hops)
        when = wanted(k, d, at, b)
        when(lambda: copy.start())
        sent.append((when, copy))

    def z_take(k, d, at):
        b = z_of(-at if d == 0 else at)
        wanted(k, d, at, b)(lambda: z_copy(k, d, at, b).wait_recv())
        if at != lasts[d] and (k == 2 or at != 4):
            z_start(k, d, at + 1, b)
        return d * 8 + at, b

    for k in (0, 1):
        for d in (0, 1):
            z_start(k, d, 1, own)
        for d in (0, 1):
            z_start(k, d, 5, own, 5)
    for d in (0, 1):
        z_start(2, d, 1, own)
    for k in (0, 1):
        y_send(k, 0, own)

    early, late = [(0, own)], [(0, own)]
    for step in range(1, 7):
        came = [(d, at) for at in (step, step + 3) for d in (0, 1) if at <= lasts[d]]
        came = [(d, at) for d, at in came if (at == step and step <= 4) or (at > 4 and at == step + 3)]
        for k in (0, 1):
            for d, at in came:
                i, b = z_take(k, d, at)
                y_send(k, i, b)
                if k == 0:
                    early.append((i, b))
        if step <= 6:
            for d in (0, 1):
                late.append(z_take(2, d, step))
        if step == 1:
            n_swap[0].wait_recv()
            n_swap[1].start()
            n_own.middle()
        if step >= 2:
            keep = len(came)
            for i, b in early[: len(early) - keep]:
                y_onward(i, b)
            early = early[len(early) - keep :]
        if step == 3:
            s_ring.middle()
        if 2 <= step <= 5:
            for i, b in late[:-2]:
                y_send(2, i, b)
            late = late[-2:]
        if step == 4:
            q_start(0)
        if step == 5:
            n_swap[1].wait_recv()
            n_other.start()
            q_pass(0)
        if step == 6:
            for i, yy in enumerate((y, left, right)):
                d_copy(0, i, yy, c).start()
            d_copy(1, 0, y, c).start()
            y_middle(1)
            for i, b in late:
                y_send(2, i, b)
            n_other.middle()
            y_finish(0)

    for copy in fetch[6:]:
        copy.wait()
    s_ring.finish()
    d_finish(0)

    for hh in (0, 1):
        total = jnp.zeros((128, 256), F32)
        for i in range(4):
            total = total + dot(sx[i], we[hh, h * 4 + i].reshape(1024, 256))
        kvp[hh] = total
        kvs[hh] = kvp[hh, far_rows].astype(BF)
    kv_swap = pass_on(1, kvs, kv_pass, kvr)
    kv_swap[0].start()
    y_finish(1)
    for d in (0, 1):
        i, b = z_take(2, d, 7)
        y_send(2, i, b)
    n_own.finish()
    kv_swap[0].wait_recv()
    kv_swap[1].start()
    q_start(1)
    i, b = z_take(2, 0, 8)
    y_send(2, i, b)
    d_copy(2, 0, y, c).start()
    d_finish(1)
    n_other.finish()
    queries = []
    for hh in (0, 1):
        queries.append(dot(nx[...], wqo[hh, :, :, :, :, 0:128].reshape(1024, 128)).astype(BF))
    kv_swap[1].wait_recv()
    first = lax.broadcasted_iota(jnp.int32, (64, 128), 1) < 64
    mix_rings = []
    for hh in (0, 1):
        both = (kvp[hh, near_rows] + kvr[hh].astype(F32)).astype(BF)
        key, value = both[:, :128], both[:, 128:]
        mixed = jnp.zeros((256, 128), F32)
        zero = jnp.zeros((64, 128), BF)
        for keep in (first, jnp.logical_not(first)):
            score = dot(queries[hh], jnp.where(keep, key, zero), NT) * (1.0 / math.sqrt(64))
            score = jnp.exp(score - jnp.max(score, axis=-1, keepdims=True))
            weight = (score / jnp.sum(score, axis=-1, keepdims=True)).astype(BF)
            mixed = mixed + dot(weight, jnp.where(keep, value, zero))
        mix[:, lanes(hh * 4 + x, 128)] = mixed.astype(BF)
        ring = wide_ring(mix, hh, 3 + hh)
        ring.start()
        mix_rings.append(ring)
    y_middle(2)
    for ring in mix_rings:
        ring.middle()
    q_pass(1)
    for ring in mix_rings:
        ring.finish()
    prev_rings = []
    for hh in (0, 1):
        at = lanes(hh * 4 + x, 128)
        out = dot(mix[...], wqo[hh, :, :, :, :, 128:256].reshape(1024, 128))
        prev[:, at] = (nx[:, at].astype(F32) + out).astype(BF)
        ring = wide_ring(prev, hh, 5 + hh)
        ring.start()
        prev_rings.append(ring)
    for ring in prev_rings:
        ring.middle()
    for ring in prev_rings:
        ring.finish()
    y_finish(2)
    d_finish(2)

    def q_wait(slot):
        for k, (ref, there) in enumerate(((q, qd), (g, gd))):
            remote(ref.at[0:64], there.at[slot], qs.at[1, k], qr.at[1 + slot, k], next_chip).wait_recv()

    @pl.when(h == 0)
    def _():
        for copy in home:
            copy.wait()

    @pl.when(h == 1)
    def _():
        q_wait(0)

    q_wait(1)

    token = lax.rem(e * 2 + h + 1, 32) * 64
    position = token + lax.broadcasted_iota(jnp.int32, (64, 128), 0)
    live = jnp.logical_and(position < lens[0], position >= 64)
    scale = 1.0 / math.sqrt(128)

    def heads(turn):
        hh, base = (1 - h if turn < 2 else h), turn % 2 * 512
        source = prev[...]
        at_key = slice(base, base + 512)
        at_value = slice(1024 + base, 1536 + base)
        keys = dot(source, wd[hh, :, :, :, :, at_key].reshape(1024, 512)).astype(BF)
        values = dot(source, wd[hh, :, :, :, :, at_value].reshape(1024, 512)).astype(BF)
        for a in range(4):
            at = slice(base + a * 128, base + a * 128 + 128)
            later = slice(1024 + base + a * 128, 1152 + base + a * 128)
            key, value = keys[:, a * 128 : a * 128 + 128], values[:, a * 128 : a * 128 + 128]
            query = qd[hh, :, at]
            score = dot(query, key, NT) * scale
            score = jnp.exp(score - jnp.max(score, axis=-1, keepdims=True))
            probs = score / jnp.sum(score, axis=-1, keepdims=True)
            low = probs.astype(BF)
            att[hh, :, at] = jnp.where(live, dot(low, value), 0.0).astype(BF)
            cot = jnp.where(live, gd[hh, :, at].astype(F32), 0.0).astype(BF)
            gkv[hh, later, :] = dot(cot, low, TN).astype(BF)
            slope = dot(cot, value, NT)
            inner = jnp.sum(slope * probs, axis=-1, keepdims=True)
            slope = (probs * (slope - inner) * scale).astype(BF)
            gkv[hh, at, :] = dot(query, slope, TN).astype(BF)

    low_rows = pl.ds(0, 64)
    on_rows = pl.ds(pl.multiple_of((1 - from_h) * 64, 64), 64)
    on_device_id = (y, (1 - from_h) * 4 + x, lax.rem(from_e + from_h, 16))
    att_far, att_direct, att_on = [], [], []
    for k in (0, 1):
        part_of = slice(k * 512, k * 512 + 512)
        att_far.append(
            remote(att.at[1 - h, :, part_of], att_pass.at[:, part_of], as_.at[k], ar.at[2 + k], next_chip)
        )
        att_direct.append(
            remote(att.at[0, :, part_of], att_out.at[low_rows, part_of], as_.at[k], ar.at[0], (y, x, after))
        )
        att_on.append(
            remote(
                att_pass.at[:, part_of], att_out.at[on_rows, part_of], as_.at[2 + k], ar.at[1 - from_h],
                on_device_id,
            )
        )
    att_near = remote(att.at[1], att_out.at[low_rows], as_.at[4], ar.at[0], (y, 4 + x, after))
    direct = jnp.logical_and(h == 1, c == 1)
    passes_att = jnp.logical_or(from_h == 0, c == 0)

    def att_start(k):
        @pl.when(direct)
        def _():
            att_direct[k].start()

        @pl.when(jnp.logical_not(direct))
        def _():
            att_far[k].start()

    def att_pass_on(k):
        @pl.when(passes_att)
        def _():
            att_far[k].wait_recv()
            att_on[k].start()

    heads(0)
    att_start(0)
    heads(1)
    att_start(1)
    heads(2)
    att_pass_on(0)
    heads(3)
    att_pass_on(1)

    @pl.when(h == 0)
    def _():
        att_out[64:128, :] = att[0]

    @pl.when(h == 1)
    def _():
        att_near.start()

    def share(to):
        total = jnp.zeros((256, 256), F32)
        for hh in (0, 1):
            rows = [
                wd[hh, lax.div(k * 4 + to, 2), pl.ds(lax.rem(to, 2) * 4, 4)].reshape(128, 2048)
                for k in (0, 1)
            ]
            total = total + dot(jnp.concatenate(rows, axis=0), gkv[hh])
        return total

    shares = []
    for m in (2, 1, 3):
        to = lax.rem(x + m, 4)
        part[m - 1] = share(to).astype(BF)
        copy = remote(part.at[m - 1], precv.at[m - 1], rs.at[m - 1], rr.at[m - 1], along_x(to))
        copy.start()
        shares.append(copy)
    gsum[...] = share(x)
    for m in (2, 1, 3):
        remote(part.at[m - 1], precv.at[m - 1], rs.at[m - 1], rr.at[m - 1], next_chip).wait_recv()
    near_cols = pl.ds(pl.multiple_of(h * 128, 128), 128)
    far_cols = pl.ds(pl.multiple_of((1 - h) * 128, 128), 128)

    def summed(cols):
        total = gsum[cols]
        for m in (1, 3, 2):
            total = total + precv[m - 1, cols].astype(F32)
        return total

    gsend[...] = summed(far_cols).astype(BF)
    g_swap = pass_on(2, gsend, g_pass, grecv)
    g_swap[0].start()
    grad_out[h] = summed(near_cols).T
    g_swap[0].wait_recv()
    g_swap[1].start()

    for when, copy in sent:
        when(copy.wait_send)
    for copy in shares:
        copy.wait_send()
    for pair in (n_swap, kv_swap, g_swap):
        for copy in pair:
            copy.wait_send()
    for ring in [s_ring, n_own, n_other] + mix_rings + prev_rings:
        ring.drain()
    for k in kinds:
        for d in (0, 1):
            ref = whole[k](y, c)
            remote(ref, ref, ys.at[k, d], yr.at[k, d], along_y(right)).wait_send()
            to = halves[k](far, d)
            remote(to, to, ys.at[k, 2 + d], yr.at[k, 2 + d], along_y(right)).wait_send()
        for i in range(4):
            d_copy(k, i, y, c).wait_send()

    @pl.when(sends_far)
    def _():
        for pair in q_to:
            pair[0].wait_send()

    @pl.when(sends_direct)
    def _():
        for pair in q_to:
            pair[1].wait_send()

    @pl.when(passes_q)
    def _():
        for copy in q_from:
            copy.wait_send()

    @pl.when(direct)
    def _():
        for copy in att_direct:
            copy.wait_send()

    @pl.when(jnp.logical_not(direct))
    def _():
        for copy in att_far:
            copy.wait_send()

    @pl.when(passes_att)
    def _():
        for copy in att_on:
            copy.wait_send()

    @pl.when(h == 1)
    def _():
        att_near.wait_send()
        remote(att.at[0], att_out.at[64:128], as_.at[0], ar.at[1], next_chip).wait_recv()

    remote(att.at[0], att_out.at[low_rows], as_.at[0], ar.at[0], next_chip).wait_recv()
    g_swap[1].wait_recv()
    grad_out[1 - h] = grecv[...].astype(F32).T


def on_device(span_states, neighbours, lengths, wq, wk, wv, wo, wkd, wvd, queries, grad_out):
    dma = pltpu.SemaphoreType.DMA
    hbm = pl.BlockSpec(memory_space=pltpu.HBM)
    vmem = pl.BlockSpec(memory_space=pltpu.VMEM)
    return pl.pallas_call(
        kernel,
        out_shape=(
            jax.ShapeDtypeStruct((128, 1024), BF),
            jax.ShapeDtypeStruct((2, 256, 128), F32),
        ),
        in_specs=[pl.BlockSpec(memory_space=pltpu.SMEM)] + [hbm] * 10,
        out_specs=(vmem, vmem),
        scratch_shapes=[
            pltpu.VMEM((2, 8, 2, 4, 128, 256), BF),
            pltpu.VMEM((2, 8, 2, 4, 16, 256), BF),
            pltpu.VMEM((2, 4, 8, 2, 16, 2048), BF),
            pltpu.VMEM((4, 128, 1024), BF),
            pltpu.VMEM((256, 1024), BF),
            pltpu.VMEM((2, 64, 1024), BF),
            pltpu.VMEM((2, 64, 1024), BF),
            pltpu.VMEM((2, 128, 256), F32),
            pltpu.VMEM((2, 64, 256), BF),
            pltpu.VMEM((2, 64, 256), BF),
            pltpu.VMEM((256, 1024), BF),
            pltpu.VMEM((256, 1024), BF),
            pltpu.VMEM((2, 2048, 256), BF),
            pltpu.VMEM((2, 64, 1024), BF),
            pltpu.VMEM((3, 256, 256), BF),
            pltpu.VMEM((3, 256, 256), BF),
            pltpu.VMEM((256, 256), F32),
            pltpu.VMEM((128, 256), BF),
            pltpu.VMEM((128, 256), BF),
            pltpu.VMEM((256, 128), BF),
            pltpu.VMEM((2, 64, 256), BF),
            pltpu.VMEM((2, 64, 1024), BF),
            pltpu.VMEM((64, 1024), BF),
            pltpu.VMEM((128, 256), BF),
            dma((10,)),
            dma((3, 2, 8)),
            dma((3, 2, 8)),
            dma((3, 4)),
            dma((3, 4)),
            dma((3, 4)),
            dma((3, 4)),
            dma((7, 4)),
            dma((7, 4)),
            dma((2, 3)),
            dma((2, 3)),
            dma((3, 2)),
            dma((3, 2)),
            dma((3,)),
            dma((3,)),
            dma((5,)),
            dma((4,)),
            dma((2, 16)),
        ],
        compiler_params=pltpu.CompilerParams(
            collective_id=0, has_side_effects=True, vmem_limit_bytes=58 * 1024 * 1024
        ),
    )(lengths, span_states, neighbours, queries, grad_out, wk, wv, wq, wo, wkd, wvd)


def solution(mesh):
    rows = P(("dp", "enc"), "tensor")
    spans = P(("dp", "enc"), None, "tensor")
    weight = P("enc", "tensor")
    return jax.shard_map(
        on_device,
        mesh=mesh,
        in_specs=(rows, spans, P("dp"), weight, weight, weight, weight, rows, rows, rows, rows),
        out_specs=(rows, spans),
        check_vma=False,
    )
```

```python
import math

import jax
import jax.numpy as jnp
from jax import lax
from jax.experimental import pallas as pl
from jax.experimental.pallas import tpu as pltpu
from jax.sharding import PartitionSpec as P

MESH = pl.DeviceIdType.MESH
BF = jnp.bfloat16
F32 = jnp.float32
NT = (((1,), (1,)), ((), ()))
TN = (((0,), (0,)), ((), ()))
NN = (((1,), (0,)), ((), ()))


def dot(a, b, dims=NN):
    return lax.dot_general(a, b, dims, preferred_element_type=F32)


def remote(src, dst, send, recv, device):
    return pltpu.make_async_remote_copy(
        src_ref=src, dst_ref=dst, send_sem=send, recv_sem=recv, device_id=device, device_id_type=MESH
    )


class Ring4:
    def __init__(self, me, device, full, half, send, recv, source=None):
        left, right, far = lax.rem(me + 3, 4), lax.rem(me + 1, 4), lax.rem(me + 2, 4)
        source = full(me) if source is None else source
        self.first = [
            remote(source, full(me), send.at[0], recv.at[0], device(right)),
            remote(source, full(me), send.at[1], recv.at[1], device(left)),
        ]
        self.arrive = [
            remote(full(left), full(left), send.at[0], recv.at[0], device(right)),
            remote(full(right), full(right), send.at[1], recv.at[1], device(left)),
        ]
        self.second = [
            remote(half(left, 0), half(left, 0), send.at[2], recv.at[2], device(right)),
            remote(half(right, 1), half(right, 1), send.at[3], recv.at[3], device(left)),
        ]
        self.last = [
            remote(half(far, 0), half(far, 0), send.at[2], recv.at[2], device(right)),
            remote(half(far, 1), half(far, 1), send.at[3], recv.at[3], device(left)),
        ]

    def start(self):
        for copy in self.first:
            copy.start()

    def middle(self):
        for k in range(2):
            self.arrive[k].wait_recv()
            self.second[k].start()

    def finish(self):
        for copy in self.last:
            copy.wait_recv()

    def drain(self):
        for copy in self.first + self.second:
            copy.wait_send()


def kernel(
    lens, s, n, q, g, wk, wv, wq, wo, wkd, wvd,
    att_out, grad_out,
    we, wqo, wd, sx, nx, qd, gd, kvp, kvs, kvr, mix, prev, gkv, att, part, precv, gsum, gsend, grecv,
    n_pass, kv_pass, qg_pass, att_pass, g_pass,
    lsem, zs, zr, ys, yr, ds, dr, xs, xr, hs, hr, qs, qr, rs, rr, as_, ar, first_came,
):
    y, t, e = lax.axis_index("dp"), lax.axis_index("tensor"), lax.axis_index("enc")
    h, x = lax.div(t, 4), lax.rem(t, 4)
    j, c = lax.div(e, 2), lax.rem(e, 2)
    z = h * 8 + j
    way = 1 - 2 * c
    before, after = lax.rem(e + 15, 16), lax.rem(e + 1, 16)
    sibling = (y, t, j * 2 + 1 - c)
    near_rows = pl.ds(pl.multiple_of(h * 64, 64), 64)
    far_rows = pl.ds(pl.multiple_of((1 - h) * 64, 64), 64)

    def along_x(i):
        return (y, h * 4 + i, e)

    def along_y(i):
        return (i, t, e)

    def z_of(k):
        zz = lax.rem(z + k + 16, 16)
        return lax.div(zz, 8), lax.rem(zz, 8)

    def along_z(k, core=c):
        hz, jz = z_of(k)
        return (y, hz * 4 + x, jz * 2 + core)

    def lanes(i, width):
        return pl.ds(pl.multiple_of(i * width, width), width)

    next_chip = along_z(way)
    onto = along_z(8 - way)
    from_h, from_j = z_of(-way)
    from_e = from_j * 2 + c

    use = pl.ds(h * 4, 4)
    blocks = (
        lambda b, yy: we.at[b[0], b[1], c, yy],
        lambda b, yy: wqo.at[b[0], b[1], c, yy],
        lambda b, yy: wd.at[b[0], yy, b[1], c],
    )
    whole = (
        lambda yy, cc: we.at[:, use, cc, yy],
        lambda yy, cc: wqo.at[:, :, cc, yy],
        lambda yy, cc: wd.at[:, yy, :, cc],
    )
    halves = (
        lambda yy, k: we.at[k, use, c, yy],
        lambda yy, k: wqo.at[k, :, c, yy],
        lambda yy, k: wd.at[k, yy, :, c],
    )
    kinds = range(3)
    own = (h, j)

    fetch = []

    def local(src, dst):
        copy = pltpu.make_async_copy(src, dst, lsem.at[len(fetch)])
        copy.start()
        fetch.append(copy)

    local(wk.at[pl.ds(y * 128, 128)], we.at[h, j, c, y, :, 0:128])
    local(wv.at[pl.ds(y * 128, 128)], we.at[h, j, c, y, :, 128:256])
    local(wq.at[pl.ds(y * 16, 16)], wqo.at[h, j, c, y, :, 0:128])
    local(wo.at[pl.ds(y * 16, 16)], wqo.at[h, j, c, y, :, 128:256])
    local(wkd, wd.at[h, y, j, c, :, 0:1024])
    local(wvd, wd.at[h, y, j, c, :, 1024:2048])
    local(s, sx.at[x])
    local(n.at[h], nx.at[:, lanes(t, 128)])

    home = [
        pltpu.make_async_copy(q.at[64:128], qd.at[0], lsem.at[8]),
        pltpu.make_async_copy(g.at[64:128], gd.at[0], lsem.at[9]),
    ]

    @pl.when(h == 0)
    def _():
        for copy in home:
            copy.start()

    barrier = pltpu.get_barrier_semaphore()

    def greet(device):
        pl.semaphore_signal(barrier, inc=1, device_id=device, device_id_type=MESH)

    for k in (7, -7):
        greet(along_z(k))
        greet(along_z(k, 1 - c))
    greet((y, 4 + x, before))

    @pl.when(h == 1)
    def _():
        greet((y, x, after))
        greet((y, 4 + x, after))

    for k in (2, 1, 3):
        greet(along_x(lax.rem(x + k, 4)))
    for k in (1, 3):
        greet(along_y(lax.rem(y + k, 4)))
    for k in (5, -5, 1, -1):
        greet(along_z(k))
    greet(sibling)
    pl.semaphore_wait(barrier, 15 + 2 * h)

    def pass_on(k, src, room, dst):
        return (
            remote(src, room, hs.at[0, k], hr.at[0, k], next_chip),
            remote(room, dst, hs.at[1, k], hr.at[1, k], onto),
        )

    n_swap = pass_on(0, n.at[1 - h], n_pass, nx.at[:, lanes(from_h * 4 + x, 128)])
    n_swap[0].start()

    def wide_ring(ref, half_of, k, source=None):
        return Ring4(
            x, along_x,
            lambda i: ref.at[:, lanes(half_of * 4 + i, 128)],
            lambda i, m: ref.at[m * 128 : m * 128 + 128, lanes(half_of * 4 + i, 128)],
            xs.at[k], xr.at[k], source,
        )

    s_ring = Ring4(
        x, along_x, lambda i: sx.at[i], lambda i, m: sx.at[i, m * 64 : m * 64 + 64], xs.at[0], xr.at[0], s
    )
    n_own = wide_ring(nx, h, 1, n.at[h])
    n_other = wide_ring(nx, 1 - h, 2)
    n_own.start()
    s_ring.start()

    for copy in fetch[:6]:
        copy.wait()

    left, right, far = lax.rem(y + 3, 4), lax.rem(y + 1, 4), lax.rem(y + 2, 4)

    def used(b):
        return pl.when(lax.div(b[1], 4) == h)

    def y_copy(k, d, i, b, yy):
        ref = blocks[k](b, yy)
        came = yr.at[k, d] if k == 1 else first_came.at[k // 2, d, i]
        return remote(ref, ref, ys.at[k, d], came, along_y(right if d == 0 else left))

    def y_send(k, i, b):
        def to_both():
            for d in (0, 1):
                y_copy(k, d, i, b, y).start()

        if k == 0:
            used(b)(to_both)
        else:
            to_both()

    def y_onward(k, i, b):
        def onward():
            for d, yy in ((0, left), (1, right)):
                y_copy(k, d, i, b, yy).wait_recv()
                ref = blocks[k](b, yy)
                width = ref.shape[-1] // 2
                ref = ref.at[:, d * width : d * width + width]
                remote(ref, ref, ys.at[k, 2 + d], yr.at[k, 2 + d], along_y(right if d == 0 else left)).start()

        if k == 0:
            used(b)(onward)
        else:
            onward()

    def d_copy(k, i, yy, cc):
        ref = whole[k](yy, cc)
        return remote(ref, ref, ds.at[k, i], dr.at[k, i], sibling)

    def y_middle(k):
        for d, yy in ((0, left), (1, right)):
            ref = whole[k](yy, c)
            remote(ref, ref, ys.at[k, d], yr.at[k, d], along_y(right)).wait_recv()
            to = halves[k](yy, d)
            remote(to, to, ys.at[k, 2 + d], yr.at[k, 2 + d], along_y(right if d == 0 else left)).start()
            d_copy(k, 1 + d, yy, c).start()

    def y_finish(k):
        for d in (0, 1):
            to = halves[k](far, d)
            remote(to, to, ys.at[k, 2 + d], yr.at[k, 2 + d], along_y(right)).wait_recv()
        d_copy(k, 3, far, c).start()

    def d_finish(k):
        for i, yy in enumerate((y, left, right, far)):
            d_copy(k, i, yy, 1 - c).wait_recv()

    q_to, q_from = [], []
    for k, (ref, there) in enumerate(((q, qd), (g, gd))):
        q_to.append((
            remote(ref.at[near_rows], qg_pass.at[k], qs.at[0, k], qr.at[0, k], next_chip),
            remote(ref.at[0:64], there.at[h], qs.at[1, k], qr.at[1 + h, k], (y, 4 + x, before)),
        ))
        q_from.append(
            remote(
                qg_pass.at[k], there.at[from_h], qs.at[2, k], qr.at[1 + from_h, k],
                (y, (1 - from_h) * 4 + x, lax.rem(from_e + 15 + from_h, 16)),
            )
        )
    sends_far = jnp.logical_or(h == 1, c == 1)
    sends_direct = jnp.logical_or(h == 1, c == 0)
    passes_q = jnp.logical_or(from_h == 1, c == 1)

    def q_start(k):
        @pl.when(sends_far)
        def _():
            q_to[k][0].start()

        @pl.when(sends_direct)
        def _():
            q_to[k][1].start()

    def q_pass(k):
        @pl.when(passes_q)
        def _():
            q_to[k][0].wait_recv()
            q_from[k].start()

    lasts = (8, 7)
    sent = []

    def z_copy(k, d, at, b, hops=1):
        ref = blocks[k](b, y)
        return remote(ref, ref, zs.at[k, d, at - 1], zr.at[k, d, at - 1], along_z(hops - 2 * hops * d))

    def wanted(k, d, at, b):
        if k != 0:
            return lambda body: body()
        end = 4 if at <= 4 else lasts[d]
        goal, some = lax.div(b[1], 4), False
        for reach in range(at, end + 1):
            there = lax.rem(b[0] * 8 + b[1] + (reach if d == 0 else 16 - reach), 16)
            some = jnp.logical_or(some, lax.div(there, 8) == goal)
        return pl.when(some)

    def z_start(k, d, at, b, hops=1):
        copy = z_copy(k, d, at, b, hops)
        when = wanted(k, d, at, b)
        when(lambda: copy.start())
        sent.append((when, copy))

    def z_take(k, d, at):
        b = z_of(-at if d == 0 else at)
        wanted(k, d, at, b)(lambda: z_copy(k, d, at, b).wait_recv())
        if at != lasts[d] and (k == 2 or at != 4):
            z_start(k, d, at + 1, b)
        return d * 8 + at, b

    for k in (0, 1):
        for d in (0, 1):
            z_start(k, d, 1, own)
        for d in (0, 1):
            z_start(k, d, 5, own, 5)
    for d in (0, 1):
        z_start(2, d, 1, own)
    for k in (0, 1):
        y_send(k, 0, own)

    early, late, gone = [(0, own)], [(0, own)], []
    for step in range(1, 7):
        came = [(d, at) for at in (step, step + 3) for d in (0, 1) if at <= lasts[d]]
        came = [(d, at) for d, at in came if (at == step and step <= 4) or (at > 4 and at == step + 3)]
        for k in (0, 1):
            for d, at in came:
                i, b = z_take(k, d, at)
                y_send(k, i, b)
                if k == 0:
                    early.append((i, b))
        if step <= 5:
            for d in (0, 1):
                late.append(z_take(2, d, step))
        if step == 1:
            n_swap[0].wait_recv()
            n_swap[1].start()
            n_own.middle()
        if step >= 2:
            keep = len(came)
            for i, b in early[: len(early) - keep]:
                y_onward(0, i, b)
            early = early[len(early) - keep :]
        if step == 3:
            s_ring.middle()
        if 2 <= step <= 5:
            for i, b in late[:-2]:
                y_send(2, i, b)
            gone, late = gone + late[:-2], late[-2:]
        if step == 4:
            q_start(0)
        if step == 5:
            n_swap[1].wait_recv()
            n_other.start()
            q_pass(0)
        if step == 6:
            for i, yy in enumerate((y, left, right)):
                d_copy(0, i, yy, c).start()
            d_copy(1, 0, y, c).start()
            y_middle(1)
            late = late + [z_take(2, d, step) for d in (0, 1)]
            for i, b in late:
                y_send(2, i, b)
            gone = gone + late
            n_other.middle()
            y_finish(0)

    for copy in fetch[6:]:
        copy.wait()
    s_ring.finish()
    d_finish(0)

    for hh in (0, 1):
        total = jnp.zeros((128, 256), F32)
        for i in range(4):
            total = total + dot(sx[i], we[hh, h * 4 + i].reshape(1024, 256))
        kvp[hh] = total
        kvs[hh] = kvp[hh, far_rows].astype(BF)
    kv_swap = pass_on(1, kvs, kv_pass, kvr)
    kv_swap[0].start()

    def late_step(step):
        took = [z_take(2, d, step) for d in (0, 1) if step <= lasts[d]]
        for i, b in took:
            y_send(2, i, b)
        return took

    y_finish(1)
    last_gone = late_step(7)
    n_own.finish()
    kv_swap[0].wait_recv()
    kv_swap[1].start()
    q_start(1)
    last_gone = last_gone + late_step(8)
    d_copy(2, 0, y, c).start()
    d_finish(1)
    n_other.finish()
    queries = []
    for hh in (0, 1):
        queries.append(dot(nx[...], wqo[hh, :, :, :, :, 0:128].reshape(1024, 128)).astype(BF))
    for i, b in gone:
        y_onward(2, i, b)
    kv_swap[1].wait_recv()
    q_pass(1)
    first = lax.broadcasted_iota(jnp.int32, (64, 128), 1) < 64
    mix_rings = []
    for hh in (0, 1):
        both = (kvp[hh, near_rows] + kvr[hh].astype(F32)).astype(BF)
        key, value = both[:, :128], both[:, 128:]
        mixed = jnp.zeros((256, 128), F32)
        zero = jnp.zeros((64, 128), BF)
        for keep in (first, jnp.logical_not(first)):
            score = dot(queries[hh], jnp.where(keep, key, zero), NT) * (1.0 / math.sqrt(64))
            score = jnp.exp(score - jnp.max(score, axis=-1, keepdims=True))
            weight = (score / jnp.sum(score, axis=-1, keepdims=True)).astype(BF)
            mixed = mixed + dot(weight, jnp.where(keep, value, zero))
        mix[:, lanes(hh * 4 + x, 128)] = mixed.astype(BF)
        ring = wide_ring(mix, hh, 3 + hh)
        ring.start()
        mix_rings.append(ring)
    for i, b in last_gone:
        y_onward(2, i, b)
    for i, yy in ((1, left), (2, right)):
        d_copy(2, i, yy, c).start()
    for ring in mix_rings:
        ring.middle()
    for ring in mix_rings:
        ring.finish()
    prev_rings = []
    for hh in (0, 1):
        at = lanes(hh * 4 + x, 128)
        out = dot(mix[...], wqo[hh, :, :, :, :, 128:256].reshape(1024, 128))
        prev[:, at] = (nx[:, at].astype(F32) + out).astype(BF)
        ring = wide_ring(prev, hh, 5 + hh)
        ring.start()
        prev_rings.append(ring)
    y_finish(2)
    for ring in prev_rings:
        ring.middle()
    for ring in prev_rings:
        ring.finish()
    d_finish(2)

    def q_wait(slot):
        for k, (ref, there) in enumerate(((q, qd), (g, gd))):
            remote(ref.at[0:64], there.at[slot], qs.at[1, k], qr.at[1 + slot, k], next_chip).wait_recv()

    @pl.when(h == 0)
    def _():
        for copy in home:
            copy.wait()

    @pl.when(h == 1)
    def _():
        q_wait(0)

    q_wait(1)

    token = lax.rem(e * 2 + h + 1, 32) * 64
    position = token + lax.broadcasted_iota(jnp.int32, (64, 128), 0)
    live = jnp.logical_and(position < lens[0], position >= 64)
    scale = 1.0 / math.sqrt(128)

    def heads(turn):
        hh, base = (1 - h if turn < 2 else h), turn % 2 * 512
        source = prev[...]
        at_key = slice(base, base + 512)
        at_value = slice(1024 + base, 1536 + base)
        keys = dot(source, wd[hh, :, :, :, :, at_key].reshape(1024, 512)).astype(BF)
        values = dot(source, wd[hh, :, :, :, :, at_value].reshape(1024, 512)).astype(BF)
        for a in range(4):
            at = slice(base + a * 128, base + a * 128 + 128)
            later = slice(1024 + base + a * 128, 1152 + base + a * 128)
            key, value = keys[:, a * 128 : a * 128 + 128], values[:, a * 128 : a * 128 + 128]
            query = qd[hh, :, at]
            score = dot(query, key, NT) * scale
            score = jnp.exp(score - jnp.max(score, axis=-1, keepdims=True))
            probs = score / jnp.sum(score, axis=-1, keepdims=True)
            low = probs.astype(BF)
            att[hh, :, at] = jnp.where(live, dot(low, value), 0.0).astype(BF)
            cot = jnp.where(live, gd[hh, :, at].astype(F32), 0.0).astype(BF)
            gkv[hh, later, :] = dot(cot, low, TN).astype(BF)
            slope = dot(cot, value, NT)
            inner = jnp.sum(slope * probs, axis=-1, keepdims=True)
            slope = (probs * (slope - inner) * scale).astype(BF)
            gkv[hh, at, :] = dot(query, slope, TN).astype(BF)

    low_rows = pl.ds(0, 64)
    on_rows = pl.ds(pl.multiple_of((1 - from_h) * 64, 64), 64)
    on_device_id = (y, (1 - from_h) * 4 + x, lax.rem(from_e + from_h, 16))
    att_far, att_direct, att_on = [], [], []
    for k in (0, 1):
        part_of = slice(k * 512, k * 512 + 512)
        att_far.append(
            remote(att.at[1 - h, :, part_of], att_pass.at[:, part_of], as_.at[k], ar.at[2 + k], next_chip)
        )
        att_direct.append(
            remote(att.at[0, :, part_of], att_out.at[low_rows, part_of], as_.at[k], ar.at[0], (y, x, after))
        )
        att_on.append(
            remote(
                att_pass.at[:, part_of], att_out.at[on_rows, part_of], as_.at[2 + k], ar.at[1 - from_h],
                on_device_id,
            )
        )
    att_near = remote(att.at[1], att_out.at[low_rows], as_.at[4], ar.at[0], (y, 4 + x, after))
    direct = jnp.logical_and(h == 1, c == 1)
    passes_att = jnp.logical_or(from_h == 0, c == 0)

    def att_start(k):
        @pl.when(direct)
        def _():
            att_direct[k].start()

        @pl.when(jnp.logical_not(direct))
        def _():
            att_far[k].start()

    def att_pass_on(k):
        @pl.when(passes_att)
        def _():
            att_far[k].wait_recv()
            att_on[k].start()

    heads(0)
    att_start(0)
    heads(1)
    att_start(1)
    heads(2)
    att_pass_on(0)
    heads(3)
    att_pass_on(1)

    @pl.when(h == 0)
    def _():
        att_out[64:128, :] = att[0]

    @pl.when(h == 1)
    def _():
        att_near.start()

    def share(to):
        total = jnp.zeros((256, 256), F32)
        for hh in (0, 1):
            rows = [
                wd[hh, lax.div(k * 4 + to, 2), pl.ds(lax.rem(to, 2) * 4, 4)].reshape(128, 2048)
                for k in (0, 1)
            ]
            total = total + dot(jnp.concatenate(rows, axis=0), gkv[hh])
        return total

    shares = []
    for m in (2, 1, 3):
        to = lax.rem(x + m, 4)
        part[m - 1] = share(to).astype(BF)
        copy = remote(part.at[m - 1], precv.at[m - 1], rs.at[m - 1], rr.at[m - 1], along_x(to))
        copy.start()
        shares.append(copy)
    gsum[...] = share(x)
    for m in (2, 1, 3):
        remote(part.at[m - 1], precv.at[m - 1], rs.at[m - 1], rr.at[m - 1], next_chip).wait_recv()
    near_cols = pl.ds(pl.multiple_of(h * 128, 128), 128)
    far_cols = pl.ds(pl.multiple_of((1 - h) * 128, 128), 128)

    def summed(cols):
        total = gsum[cols]
        for m in (1, 3, 2):
            total = total + precv[m - 1, cols].astype(F32)
        return total

    gsend[...] = summed(far_cols).astype(BF)
    g_swap = pass_on(2, gsend, g_pass, grecv)
    g_swap[0].start()
    grad_out[h] = summed(near_cols).T
    g_swap[0].wait_recv()
    g_swap[1].start()

    for when, copy in sent:
        when(copy.wait_send)
    for copy in shares:
        copy.wait_send()
    for pair in (n_swap, kv_swap, g_swap):
        for copy in pair:
            copy.wait_send()
    for ring in [s_ring, n_own, n_other] + mix_rings + prev_rings:
        ring.drain()
    for k in kinds:
        for d in (0, 1):
            ref = whole[k](y, c)
            remote(ref, ref, ys.at[k, d], yr.at[k, d], along_y(right)).wait_send()
            to = halves[k](far, d)
            remote(to, to, ys.at[k, 2 + d], yr.at[k, 2 + d], along_y(right)).wait_send()
        for i in range(4):
            d_copy(k, i, y, c).wait_send()

    @pl.when(sends_far)
    def _():
        for pair in q_to:
            pair[0].wait_send()

    @pl.when(sends_direct)
    def _():
        for pair in q_to:
            pair[1].wait_send()

    @pl.when(passes_q)
    def _():
        for copy in q_from:
            copy.wait_send()

    @pl.when(direct)
    def _():
        for copy in att_direct:
            copy.wait_send()

    @pl.when(jnp.logical_not(direct))
    def _():
        for copy in att_far:
            copy.wait_send()

    @pl.when(passes_att)
    def _():
        for copy in att_on:
            copy.wait_send()

    @pl.when(h == 1)
    def _():
        att_near.wait_send()
        remote(att.at[0], att_out.at[64:128], as_.at[0], ar.at[1], next_chip).wait_recv()

    remote(att.at[0], att_out.at[low_rows], as_.at[0], ar.at[0], next_chip).wait_recv()
    g_swap[1].wait_recv()
    grad_out[1 - h] = grecv[...].astype(F32).T


def on_device(span_states, neighbours, lengths, wq, wk, wv, wo, wkd, wvd, queries, grad_out):
    dma = pltpu.SemaphoreType.DMA
    hbm = pl.BlockSpec(memory_space=pltpu.HBM)
    vmem = pl.BlockSpec(memory_space=pltpu.VMEM)
    return pl.pallas_call(
        kernel,
        out_shape=(
            jax.ShapeDtypeStruct((128, 1024), BF),
            jax.ShapeDtypeStruct((2, 256, 128), F32),
        ),
        in_specs=[pl.BlockSpec(memory_space=pltpu.SMEM)] + [hbm] * 10,
        out_specs=(vmem, vmem),
        scratch_shapes=[
            pltpu.VMEM((2, 8, 2, 4, 128, 256), BF),
            pltpu.VMEM((2, 8, 2, 4, 16, 256), BF),
            pltpu.VMEM((2, 4, 8, 2, 16, 2048), BF),
            pltpu.VMEM((4, 128, 1024), BF),
            pltpu.VMEM((256, 1024), BF),
            pltpu.VMEM((2, 64, 1024), BF),
            pltpu.VMEM((2, 64, 1024), BF),
            pltpu.VMEM((2, 128, 256), F32),
            pltpu.VMEM((2, 64, 256), BF),
            pltpu.VMEM((2, 64, 256), BF),
            pltpu.VMEM((256, 1024), BF),
            pltpu.VMEM((256, 1024), BF),
            pltpu.VMEM((2, 2048, 256), BF),
            pltpu.VMEM((2, 64, 1024), BF),
            pltpu.VMEM((3, 256, 256), BF),
            pltpu.VMEM((3, 256, 256), BF),
            pltpu.VMEM((256, 256), F32),
            pltpu.VMEM((128, 256), BF),
            pltpu.VMEM((128, 256), BF),
            pltpu.VMEM((256, 128), BF),
            pltpu.VMEM((2, 64, 256), BF),
            pltpu.VMEM((2, 64, 1024), BF),
            pltpu.VMEM((64, 1024), BF),
            pltpu.VMEM((128, 256), BF),
            dma((10,)),
            dma((3, 2, 8)),
            dma((3, 2, 8)),
            dma((3, 4)),
            dma((3, 4)),
            dma((3, 4)),
            dma((3, 4)),
            dma((7, 4)),
            dma((7, 4)),
            dma((2, 3)),
            dma((2, 3)),
            dma((3, 2)),
            dma((3, 2)),
            dma((3,)),
            dma((3,)),
            dma((5,)),
            dma((4,)),
            dma((2, 2, 16)),
        ],
        compiler_params=pltpu.CompilerParams(
            collective_id=0, has_side_effects=True, vmem_limit_bytes=58 * 1024 * 1024
        ),
    )(lengths, span_states, neighbours, queries, grad_out, wk, wv, wq, wo, wkd, wvd)


def solution(mesh):
    rows = P(("dp", "enc"), "tensor")
    spans = P(("dp", "enc"), None, "tensor")
    weight = P("enc", "tensor")
    return jax.shard_map(
        on_device,
        mesh=mesh,
        in_specs=(rows, spans, P("dp"), weight, weight, weight, weight, rows, rows, rows, rows),
        out_specs=(rows, spans),
        check_vma=False,
    )
```

```python
import math

import jax
import jax.numpy as jnp
from jax import lax
from jax.experimental import pallas as pl
from jax.experimental.pallas import tpu as pltpu
from jax.sharding import PartitionSpec as P

MESH = pl.DeviceIdType.MESH
BF = jnp.bfloat16
F32 = jnp.float32
NT = (((1,), (1,)), ((), ()))
TN = (((0,), (0,)), ((), ()))
NN = (((1,), (0,)), ((), ()))


def dot(a, b, dims=NN):
    return lax.dot_general(a, b, dims, preferred_element_type=F32)


def remote(src, dst, send, recv, device):
    return pltpu.make_async_remote_copy(
        src_ref=src, dst_ref=dst, send_sem=send, recv_sem=recv, device_id=device, device_id_type=MESH
    )


class Ring4:
    def __init__(self, me, device, full, half, send, recv, source=None):
        left, right, far = lax.rem(me + 3, 4), lax.rem(me + 1, 4), lax.rem(me + 2, 4)
        source = full(me) if source is None else source
        self.first = [
            remote(source, full(me), send.at[0], recv.at[0], device(right)),
            remote(source, full(me), send.at[1], recv.at[1], device(left)),
        ]
        self.arrive = [
            remote(full(left), full(left), send.at[0], recv.at[0], device(right)),
            remote(full(right), full(right), send.at[1], recv.at[1], device(left)),
        ]
        self.second = [
            remote(half(left, 0), half(left, 0), send.at[2], recv.at[2], device(right)),
            remote(half(right, 1), half(right, 1), send.at[3], recv.at[3], device(left)),
        ]
        self.last = [
            remote(half(far, 0), half(far, 0), send.at[2], recv.at[2], device(right)),
            remote(half(far, 1), half(far, 1), send.at[3], recv.at[3], device(left)),
        ]

    def start(self):
        for copy in self.first:
            copy.start()

    def middle(self):
        for k in range(2):
            self.arrive[k].wait_recv()
            self.second[k].start()

    def finish(self):
        for copy in self.last:
            copy.wait_recv()

    def drain(self):
        for copy in self.first + self.second:
            copy.wait_send()


def kernel(
    lens, s, n, q, g, wk, wv, wq, wo, wkd, wvd,
    att_out, grad_out,
    we, wqo, wd, sx, nx, qd, gd, kvp, kvs, kvr, mix, prev, gkv, att, part, precv, gsum, gsend, grecv,
    n_pass, kv_pass, qg_pass, att_pass, g_pass,
    lsem, zs, zr, ys, yr, ds, dr, xs, xr, hs, hr, qs, qr, rs, rr, as_, ar, first_came,
):
    y, t, e = lax.axis_index("dp"), lax.axis_index("tensor"), lax.axis_index("enc")
    h, x = lax.div(t, 4), lax.rem(t, 4)
    j, c = lax.div(e, 2), lax.rem(e, 2)
    z = h * 8 + j
    way = 1 - 2 * c
    before, after = lax.rem(e + 15, 16), lax.rem(e + 1, 16)
    sibling = (y, t, j * 2 + 1 - c)
    near_rows = pl.ds(pl.multiple_of(h * 64, 64), 64)
    far_rows = pl.ds(pl.multiple_of((1 - h) * 64, 64), 64)

    def along_x(i):
        return (y, h * 4 + i, e)

    def along_y(i):
        return (i, t, e)

    def z_of(k):
        zz = lax.rem(z + k + 16, 16)
        return lax.div(zz, 8), lax.rem(zz, 8)

    def along_z(k, core=c):
        hz, jz = z_of(k)
        return (y, hz * 4 + x, jz * 2 + core)

    def lanes(i, width):
        return pl.ds(pl.multiple_of(i * width, width), width)

    next_chip = along_z(way)
    onto = along_z(8 - way)
    from_h, from_j = z_of(-way)
    from_e = from_j * 2 + c
    out_chip = along_z(7 * way)
    out_onto = along_z(way)
    out_h, out_j = z_of(-7 * way)
    out_e = out_j * 2 + c

    use = pl.ds(h * 4, 4)
    blocks = (
        lambda b, yy: we.at[b[0], b[1], c, yy],
        lambda b, yy: wqo.at[b[0], b[1], c, yy],
        lambda b, yy: wd.at[b[0], yy, b[1], c],
    )
    whole = (
        lambda yy, cc: we.at[:, use, cc, yy],
        lambda yy, cc: wqo.at[:, :, cc, yy],
        lambda yy, cc: wd.at[:, yy, :, cc],
    )
    halves = (
        lambda yy, k: we.at[k, use, c, yy],
        lambda yy, k: wqo.at[k, :, c, yy],
        lambda yy, k: wd.at[k, yy, :, c],
    )
    kinds = range(3)
    own = (h, j)

    fetch = []

    def local(src, dst):
        copy = pltpu.make_async_copy(src, dst, lsem.at[len(fetch)])
        copy.start()
        fetch.append(copy)

    local(wk.at[pl.ds(y * 128, 128)], we.at[h, j, c, y, :, 0:128])
    local(wv.at[pl.ds(y * 128, 128)], we.at[h, j, c, y, :, 128:256])
    local(wq.at[pl.ds(y * 16, 16)], wqo.at[h, j, c, y, :, 0:128])
    local(wo.at[pl.ds(y * 16, 16)], wqo.at[h, j, c, y, :, 128:256])
    local(wkd, wd.at[h, y, j, c, :, 0:1024])
    local(wvd, wd.at[h, y, j, c, :, 1024:2048])
    local(s, sx.at[x])
    local(n.at[h], nx.at[:, lanes(t, 128)])

    home = [
        pltpu.make_async_copy(q.at[64:128], qd.at[0], lsem.at[8]),
        pltpu.make_async_copy(g.at[64:128], gd.at[0], lsem.at[9]),
    ]

    @pl.when(h == 0)
    def _():
        for copy in home:
            copy.start()

    barrier = pltpu.get_barrier_semaphore()

    def greet(device):
        pl.semaphore_signal(barrier, inc=1, device_id=device, device_id_type=MESH)

    for k in (7, -7):
        greet(along_z(k))
        greet(along_z(k, 1 - c))
    greet((y, 4 + x, before))

    @pl.when(h == 1)
    def _():
        greet((y, x, after))
        greet((y, 4 + x, after))

    for k in (2, 1, 3):
        greet(along_x(lax.rem(x + k, 4)))
    for k in (1, 3):
        greet(along_y(lax.rem(y + k, 4)))
    for k in (1, -1):
        greet(along_z(k, 1 - c))
    for k in (5, -5, 1, -1):
        greet(along_z(k))
    greet(sibling)
    pl.semaphore_wait(barrier, 17 + 2 * h)

    def pass_on(k, src, room, dst, relay=next_chip, end=onto):
        return (
            remote(src, room, hs.at[0, k], hr.at[0, k], relay),
            remote(room, dst, hs.at[1, k], hr.at[1, k], end),
        )

    n_swap = pass_on(0, n.at[1 - h], n_pass, nx.at[:, lanes(from_h * 4 + x, 128)])
    n_swap[0].start()

    def wide_ring(ref, half_of, k, source=None):
        return Ring4(
            x, along_x,
            lambda i: ref.at[:, lanes(half_of * 4 + i, 128)],
            lambda i, m: ref.at[m * 128 : m * 128 + 128, lanes(half_of * 4 + i, 128)],
            xs.at[k], xr.at[k], source,
        )

    s_ring = Ring4(
        x, along_x, lambda i: sx.at[i], lambda i, m: sx.at[i, m * 64 : m * 64 + 64], xs.at[0], xr.at[0], s
    )
    n_own = wide_ring(nx, h, 1, n.at[h])
    n_other = wide_ring(nx, 1 - h, 2)
    n_own.start()
    s_ring.start()

    for copy in fetch[:6]:
        copy.wait()

    left, right, far = lax.rem(y + 3, 4), lax.rem(y + 1, 4), lax.rem(y + 2, 4)

    def used(b):
        return pl.when(lax.div(b[1], 4) == h)

    def y_copy(k, d, i, b, yy):
        ref = blocks[k](b, yy)
        came = yr.at[k, d] if k == 1 else first_came.at[k // 2, d, i]
        return remote(ref, ref, ys.at[k, d], came, along_y(right if d == 0 else left))

    def y_send(k, i, b):
        def to_both():
            for d in (0, 1):
                y_copy(k, d, i, b, y).start()

        if k == 0:
            used(b)(to_both)
        else:
            to_both()

    def y_onward(k, i, b):
        def onward():
            for d, yy in ((0, left), (1, right)):
                y_copy(k, d, i, b, yy).wait_recv()
                ref = blocks[k](b, yy)
                width = ref.shape[-1] // 2
                ref = ref.at[:, d * width : d * width + width]
                remote(ref, ref, ys.at[k, 2 + d], yr.at[k, 2 + d], along_y(right if d == 0 else left)).start()

        if k == 0:
            used(b)(onward)
        else:
            onward()

    def d_copy(k, i, yy, cc):
        ref = whole[k](yy, cc)
        return remote(ref, ref, ds.at[k, i], dr.at[k, i], sibling)

    def y_middle(k):
        for d, yy in ((0, left), (1, right)):
            ref = whole[k](yy, c)
            remote(ref, ref, ys.at[k, d], yr.at[k, d], along_y(right)).wait_recv()
            to = halves[k](yy, d)
            remote(to, to, ys.at[k, 2 + d], yr.at[k, 2 + d], along_y(right if d == 0 else left)).start()
            d_copy(k, 1 + d, yy, c).start()

    def y_finish(k):
        for d in (0, 1):
            to = halves[k](far, d)
            remote(to, to, ys.at[k, 2 + d], yr.at[k, 2 + d], along_y(right)).wait_recv()
        d_copy(k, 3, far, c).start()

    def d_finish(k):
        for i, yy in enumerate((y, left, right, far)):
            d_copy(k, i, yy, 1 - c).wait_recv()

    q_to, q_from = [], []
    for k, (ref, there) in enumerate(((q, qd), (g, gd))):
        q_to.append((
            remote(ref.at[near_rows], qg_pass.at[k], qs.at[0, k], qr.at[0, k], next_chip),
            remote(ref.at[0:64], there.at[h], qs.at[1, k], qr.at[1 + h, k], (y, 4 + x, before)),
        ))
        q_from.append(
            remote(
                qg_pass.at[k], there.at[from_h], qs.at[2, k], qr.at[1 + from_h, k],
                (y, (1 - from_h) * 4 + x, lax.rem(from_e + 15 + from_h, 16)),
            )
        )
    sends_far = jnp.logical_or(h == 1, c == 1)
    sends_direct = jnp.logical_or(h == 1, c == 0)
    passes_q = jnp.logical_or(from_h == 1, c == 1)

    def q_start(k):
        @pl.when(sends_far)
        def _():
            q_to[k][0].start()

        @pl.when(sends_direct)
        def _():
            q_to[k][1].start()

    def q_pass(k):
        @pl.when(passes_q)
        def _():
            q_to[k][0].wait_recv()
            q_from[k].start()

    lasts = (8, 7)
    sent = []

    def z_copy(k, d, at, b, hops=1):
        ref = blocks[k](b, y)
        return remote(ref, ref, zs.at[k, d, at - 1], zr.at[k, d, at - 1], along_z(hops - 2 * hops * d))

    def wanted(k, d, at, b):
        if k != 0:
            return lambda body: body()
        end = 4 if at <= 4 else lasts[d]
        goal, some = lax.div(b[1], 4), False
        for reach in range(at, end + 1):
            there = lax.rem(b[0] * 8 + b[1] + (reach if d == 0 else 16 - reach), 16)
            some = jnp.logical_or(some, lax.div(there, 8) == goal)
        return pl.when(some)

    def z_start(k, d, at, b, hops=1):
        copy = z_copy(k, d, at, b, hops)
        when = wanted(k, d, at, b)
        when(lambda: copy.start())
        sent.append((when, copy))

    def z_take(k, d, at):
        b = z_of(-at if d == 0 else at)
        wanted(k, d, at, b)(lambda: z_copy(k, d, at, b).wait_recv())
        if at != lasts[d] and (k == 2 or at != 4):
            z_start(k, d, at + 1, b)
        return d * 8 + at, b

    for k in (0, 1):
        for d in (0, 1):
            z_start(k, d, 1, own)
        for d in (0, 1):
            z_start(k, d, 5, own, 5)
    for d in (0, 1):
        z_start(2, d, 1, own)
    for k in (0, 1):
        y_send(k, 0, own)

    early, late, gone = [(0, own)], [(0, own)], []
    for step in range(1, 7):
        came = [(d, at) for at in (step, step + 3) for d in (0, 1) if at <= lasts[d]]
        came = [(d, at) for d, at in came if (at == step and step <= 4) or (at > 4 and at == step + 3)]
        for k in (0, 1):
            for d, at in came:
                i, b = z_take(k, d, at)
                y_send(k, i, b)
                if k == 0:
                    early.append((i, b))
        if step <= 5:
            for d in (0, 1):
                late.append(z_take(2, d, step))
        if step == 1:
            n_swap[0].wait_recv()
            n_swap[1].start()
            n_own.middle()
        if step >= 2:
            keep = len(came)
            for i, b in early[: len(early) - keep]:
                y_onward(0, i, b)
            early = early[len(early) - keep :]
        if step == 3:
            s_ring.middle()
        if 2 <= step <= 5:
            for i, b in late[:-2]:
                y_send(2, i, b)
            gone, late = gone + late[:-2], late[-2:]
        if step == 4:
            q_start(0)
        if step == 5:
            n_swap[1].wait_recv()
            n_other.start()
            q_pass(0)
        if step == 6:
            for i, yy in enumerate((y, left, right)):
                d_copy(0, i, yy, c).start()
            d_copy(1, 0, y, c).start()
            y_middle(1)
            late = late + [z_take(2, d, step) for d in (0, 1)]
            for i, b in late:
                y_send(2, i, b)
            gone = gone + late
            n_other.middle()
            y_finish(0)

    for copy in fetch[6:]:
        copy.wait()
    s_ring.finish()
    d_finish(0)

    for hh in (0, 1):
        total = jnp.zeros((128, 256), F32)
        for i in range(4):
            total = total + dot(sx[i], we[hh, h * 4 + i].reshape(1024, 256))
        kvp[hh] = total
        kvs[hh] = kvp[hh, far_rows].astype(BF)
    kv_swap = pass_on(1, kvs, kv_pass, kvr)
    kv_swap[0].start()

    def late_step(step):
        took = [z_take(2, d, step) for d in (0, 1) if step <= lasts[d]]
        for i, b in took:
            y_send(2, i, b)
        return took

    y_finish(1)
    last_gone = late_step(7)
    n_own.finish()
    kv_swap[0].wait_recv()
    kv_swap[1].start()
    q_start(1)
    last_gone = last_gone + late_step(8)
    d_copy(2, 0, y, c).start()
    d_finish(1)
    n_other.finish()
    queries = []
    for hh in (0, 1):
        queries.append(dot(nx[...], wqo[hh, :, :, :, :, 0:128].reshape(1024, 128)).astype(BF))
    for i, b in gone:
        y_onward(2, i, b)
    kv_swap[1].wait_recv()
    q_pass(1)
    first = lax.broadcasted_iota(jnp.int32, (64, 128), 1) < 64
    mix_rings = []
    for hh in (0, 1):
        both = (kvp[hh, near_rows] + kvr[hh].astype(F32)).astype(BF)
        key, value = both[:, :128], both[:, 128:]
        mixed = jnp.zeros((256, 128), F32)
        zero = jnp.zeros((64, 128), BF)
        for keep in (first, jnp.logical_not(first)):
            score = dot(queries[hh], jnp.where(keep, key, zero), NT) * (1.0 / math.sqrt(64))
            score = jnp.exp(score - jnp.max(score, axis=-1, keepdims=True))
            weight = (score / jnp.sum(score, axis=-1, keepdims=True)).astype(BF)
            mixed = mixed + dot(weight, jnp.where(keep, value, zero))
        mix[:, lanes(hh * 4 + x, 128)] = mixed.astype(BF)
        ring = wide_ring(mix, hh, 3 + hh)
        ring.start()
        mix_rings.append(ring)
    for i, b in last_gone:
        y_onward(2, i, b)
    for i, yy in ((1, left), (2, right)):
        d_copy(2, i, yy, c).start()
    for ring in mix_rings:
        ring.middle()
    for ring in mix_rings:
        ring.finish()
    prev_rings = []
    for hh in (0, 1):
        at = lanes(hh * 4 + x, 128)
        out = dot(mix[...], wqo[hh, :, :, :, :, 128:256].reshape(1024, 128))
        prev[:, at] = (nx[:, at].astype(F32) + out).astype(BF)
        ring = wide_ring(prev, hh, 5 + hh)
        ring.start()
        prev_rings.append(ring)
    y_finish(2)
    for ring in prev_rings:
        ring.middle()
    for ring in prev_rings:
        ring.finish()
    d_finish(2)

    def q_wait(slot):
        for k, (ref, there) in enumerate(((q, qd), (g, gd))):
            remote(ref.at[0:64], there.at[slot], qs.at[1, k], qr.at[1 + slot, k], next_chip).wait_recv()

    @pl.when(h == 0)
    def _():
        for copy in home:
            copy.wait()

    @pl.when(h == 1)
    def _():
        q_wait(0)

    q_wait(1)

    token = lax.rem(e * 2 + h + 1, 32) * 64
    position = token + lax.broadcasted_iota(jnp.int32, (64, 128), 0)
    live = jnp.logical_and(position < lens[0], position >= 64)
    scale = 1.0 / math.sqrt(128)

    def heads(turn):
        hh, base = (1 - h if turn < 2 else h), turn % 2 * 512
        source = prev[...]
        at_key = slice(base, base + 512)
        at_value = slice(1024 + base, 1536 + base)
        keys = dot(source, wd[hh, :, :, :, :, at_key].reshape(1024, 512)).astype(BF)
        values = dot(source, wd[hh, :, :, :, :, at_value].reshape(1024, 512)).astype(BF)
        for a in range(4):
            at = slice(base + a * 128, base + a * 128 + 128)
            later = slice(1024 + base + a * 128, 1152 + base + a * 128)
            key, value = keys[:, a * 128 : a * 128 + 128], values[:, a * 128 : a * 128 + 128]
            query = qd[hh, :, at]
            score = dot(query, key, NT) * scale
            score = jnp.exp(score - jnp.max(score, axis=-1, keepdims=True))
            probs = score / jnp.sum(score, axis=-1, keepdims=True)
            low = probs.astype(BF)
            att[hh, :, at] = jnp.where(live, dot(low, value), 0.0).astype(BF)
            cot = jnp.where(live, gd[hh, :, at].astype(F32), 0.0).astype(BF)
            gkv[hh, later, :] = dot(cot, low, TN).astype(BF)
            slope = dot(cot, value, NT)
            inner = jnp.sum(slope * probs, axis=-1, keepdims=True)
            slope = (probs * (slope - inner) * scale).astype(BF)
            gkv[hh, at, :] = dot(query, slope, TN).astype(BF)

    low_rows = pl.ds(0, 64)
    on_rows = pl.ds(pl.multiple_of((1 - out_h) * 64, 64), 64)
    on_device_id = (y, (1 - out_h) * 4 + x, lax.rem(out_e + out_h, 16))
    att_far, att_direct, att_on = [], [], []
    for k in (0, 1):
        part_of = slice(k * 512, k * 512 + 512)
        att_far.append(
            remote(att.at[1 - h, :, part_of], att_pass.at[:, part_of], as_.at[k], ar.at[2 + k], out_chip)
        )
        att_direct.append(
            remote(att.at[0, :, part_of], att_out.at[low_rows, part_of], as_.at[k], ar.at[0], (y, x, after))
        )
        att_on.append(
            remote(
                att_pass.at[:, part_of], att_out.at[on_rows, part_of], as_.at[2 + k], ar.at[1 - out_h],
                on_device_id,
            )
        )
    att_near = remote(att.at[1], att_out.at[low_rows], as_.at[4], ar.at[0], (y, 4 + x, after))
    direct = jnp.logical_and(h == 1, c == 1)
    passes_att = jnp.logical_or(out_h == 0, c == 0)

    def att_start(k):
        @pl.when(direct)
        def _():
            att_direct[k].start()

        @pl.when(jnp.logical_not(direct))
        def _():
            att_far[k].start()

    def att_pass_on(k):
        @pl.when(passes_att)
        def _():
            att_far[k].wait_recv()
            att_on[k].start()

    heads(0)
    att_start(0)
    heads(1)
    att_start(1)
    heads(2)
    heads(3)

    @pl.when(h == 0)
    def _():
        att_out[64:128, :] = att[0]

    @pl.when(h == 1)
    def _():
        att_near.start()

    def share(to):
        total = jnp.zeros((256, 256), F32)
        for hh in (0, 1):
            rows = [
                wd[hh, lax.div(k * 4 + to, 2), pl.ds(lax.rem(to, 2) * 4, 4)].reshape(128, 2048)
                for k in (0, 1)
            ]
            total = total + dot(jnp.concatenate(rows, axis=0), gkv[hh])
        return total

    shares = []
    for m in (2, 1, 3):
        to = lax.rem(x + m, 4)
        part[m - 1] = share(to).astype(BF)
        copy = remote(part.at[m - 1], precv.at[m - 1], rs.at[m - 1], rr.at[m - 1], along_x(to))
        copy.start()
        shares.append(copy)
    gsum[...] = share(x)
    att_pass_on(0)
    att_pass_on(1)
    for m in (2, 1, 3):
        remote(part.at[m - 1], precv.at[m - 1], rs.at[m - 1], rr.at[m - 1], next_chip).wait_recv()
    near_cols = pl.ds(pl.multiple_of(h * 128, 128), 128)
    far_cols = pl.ds(pl.multiple_of((1 - h) * 128, 128), 128)

    def summed(cols):
        total = gsum[cols]
        for m in (1, 3, 2):
            total = total + precv[m - 1, cols].astype(F32)
        return total

    gsend[...] = summed(far_cols).astype(BF)
    g_swap = pass_on(2, gsend, g_pass, grecv, out_chip, out_onto)
    g_swap[0].start()
    grad_out[h] = summed(near_cols).T
    g_swap[0].wait_recv()
    g_swap[1].start()

    for when, copy in sent:
        when(copy.wait_send)
    for copy in shares:
        copy.wait_send()
    for pair in (n_swap, kv_swap, g_swap):
        for copy in pair:
            copy.wait_send()
    for ring in [s_ring, n_own, n_other] + mix_rings + prev_rings:
        ring.drain()
    for k in kinds:
        for d in (0, 1):
            ref = whole[k](y, c)
            remote(ref, ref, ys.at[k, d], yr.at[k, d], along_y(right)).wait_send()
            to = halves[k](far, d)
            remote(to, to, ys.at[k, 2 + d], yr.at[k, 2 + d], along_y(right)).wait_send()
        for i in range(4):
            d_copy(k, i, y, c).wait_send()

    @pl.when(sends_far)
    def _():
        for pair in q_to:
            pair[0].wait_send()

    @pl.when(sends_direct)
    def _():
        for pair in q_to:
            pair[1].wait_send()

    @pl.when(passes_q)
    def _():
        for copy in q_from:
            copy.wait_send()

    @pl.when(direct)
    def _():
        for copy in att_direct:
            copy.wait_send()

    @pl.when(jnp.logical_not(direct))
    def _():
        for copy in att_far:
            copy.wait_send()

    @pl.when(passes_att)
    def _():
        for copy in att_on:
            copy.wait_send()

    @pl.when(h == 1)
    def _():
        att_near.wait_send()
        remote(att.at[0], att_out.at[64:128], as_.at[0], ar.at[1], next_chip).wait_recv()

    remote(att.at[0], att_out.at[low_rows], as_.at[0], ar.at[0], next_chip).wait_recv()
    g_swap[1].wait_recv()
    grad_out[1 - h] = grecv[...].astype(F32).T


def on_device(span_states, neighbours, lengths, wq, wk, wv, wo, wkd, wvd, queries, grad_out):
    dma = pltpu.SemaphoreType.DMA
    hbm = pl.BlockSpec(memory_space=pltpu.HBM)
    vmem = pl.BlockSpec(memory_space=pltpu.VMEM)
    return pl.pallas_call(
        kernel,
        out_shape=(
            jax.ShapeDtypeStruct((128, 1024), BF),
            jax.ShapeDtypeStruct((2, 256, 128), F32),
        ),
        in_specs=[pl.BlockSpec(memory_space=pltpu.SMEM)] + [hbm] * 10,
        out_specs=(vmem, vmem),
        scratch_shapes=[
            pltpu.VMEM((2, 8, 2, 4, 128, 256), BF),
            pltpu.VMEM((2, 8, 2, 4, 16, 256), BF),
            pltpu.VMEM((2, 4, 8, 2, 16, 2048), BF),
            pltpu.VMEM((4, 128, 1024), BF),
            pltpu.VMEM((256, 1024), BF),
            pltpu.VMEM((2, 64, 1024), BF),
            pltpu.VMEM((2, 64, 1024), BF),
            pltpu.VMEM((2, 128, 256), F32),
            pltpu.VMEM((2, 64, 256), BF),
            pltpu.VMEM((2, 64, 256), BF),
            pltpu.VMEM((256, 1024), BF),
            pltpu.VMEM((256, 1024), BF),
            pltpu.VMEM((2, 2048, 256), BF),
            pltpu.VMEM((2, 64, 1024), BF),
            pltpu.VMEM((3, 256, 256), BF),
            pltpu.VMEM((3, 256, 256), BF),
            pltpu.VMEM((256, 256), F32),
            pltpu.VMEM((128, 256), BF),
            pltpu.VMEM((128, 256), BF),
            pltpu.VMEM((256, 128), BF),
            pltpu.VMEM((2, 64, 256), BF),
            pltpu.VMEM((2, 64, 1024), BF),
            pltpu.VMEM((64, 1024), BF),
            pltpu.VMEM((128, 256), BF),
            dma((10,)),
            dma((3, 2, 8)),
            dma((3, 2, 8)),
            dma((3, 4)),
            dma((3, 4)),
            dma((3, 4)),
            dma((3, 4)),
            dma((7, 4)),
            dma((7, 4)),
            dma((2, 3)),
            dma((2, 3)),
            dma((3, 2)),
            dma((3, 2)),
            dma((3,)),
            dma((3,)),
            dma((5,)),
            dma((4,)),
            dma((2, 2, 16)),
        ],
        compiler_params=pltpu.CompilerParams(
            collective_id=0, has_side_effects=True, vmem_limit_bytes=58 * 1024 * 1024
        ),
    )(lengths, span_states, neighbours, queries, grad_out, wk, wv, wq, wo, wkd, wvd)


def solution(mesh):
    rows = P(("dp", "enc"), "tensor")
    spans = P(("dp", "enc"), None, "tensor")
    weight = P("enc", "tensor")
    return jax.shard_map(
        on_device,
        mesh=mesh,
        in_specs=(rows, spans, P("dp"), weight, weight, weight, weight, rows, rows, rows, rows),
        out_specs=(rows, spans),
        check_vma=False,
    )
```
